32 devices in a mesh: rep: 1, dp: 32 (over x, y, z, core).
Axes of the slice: x: 2, y: 2, z: 4, core: 2. Of those that a mesh axis runs over, the one named last changes fastest.
Arguments:
- x: bfloat16 [32, 2048, 768], P(('rep', 'dp'))
- dy: bfloat16 [32, 2048, 768], P(('rep', 'dp'))
- w_gate: bfloat16 [2, 768, 1792], P(None, 'dp')
- w_up: bfloat16 [2, 768, 1792], P(None, 'dp')
- w_down: bfloat16 [2, 1792, 768], P(None, 'dp')
Outputs:
- output 1: bfloat16 [32, 2048, 768], P(('rep', 'dp'))
- output 2: bfloat16 [2, 768, 1792], P('rep', 'dp')
- output 3: bfloat16 [2, 768, 1792], P('rep', 'dp')
- output 4: bfloat16 [2, 1792, 768], P('rep', 'dp')
All inputs are finite; a program needn't handle non-finite values.
Results may differ from the reference program's by a relative error of at most 0.018.
Values are sent between devices in bfloat16 or wider.
A program may use at most 2 GiB of HBM per device.

```python
import jax
import jax.numpy as jnp
from jax import lax

SEQUENCES = 32
TOKENS = 2048
D = 768
FF = 1792
LAYERS = 2
NAMES = ("w_gate", "w_up", "w_down")
SHAPES = {"w_gate": (LAYERS, D, FF), "w_up": (LAYERS, D, FF), "w_down": (LAYERS, FF, D)}


def bump(key, n, height):
    away = (jnp.arange(n, dtype=jnp.int32) - jax.random.randint(key, (), 0, n, jnp.int32)) % n
    return jnp.where(away < n // 8, height, 1.0)


def together(key, own, strength):
    shared = jax.random.normal(key, own.shape[1:], jnp.float32)
    return (own + strength * shared) * lax.rsqrt(1 + strength * strength)


def setup_inputs(seed: int = 0, part: int = 0) -> dict:
    kx, kdy, ka, kb, kz, kf, kh, kl, *kw = jax.random.split(jax.random.key(seed), 8 + len(NAMES))
    kx, kdy, ka, kb = (jax.random.fold_in(k, part) for k in (kx, kdy, ka, kb))
    shape = (SEQUENCES, TOKENS, D)
    much_x, much_dy = jax.random.uniform(kz, (2,), jnp.float32, 0.0, 1.0)
    layers = 2.0 ** jax.random.uniform(kl, (LAYERS, 1, 1), jnp.float32, -1.0, 1.0)
    x = together(ka, jax.random.normal(kx, shape, jnp.float32), much_x) * bump(kf, D, 4.0)
    dy = together(kb, jax.random.normal(kdy, shape, jnp.float32), much_dy)
    drawn = {"x": x.astype(jnp.bfloat16), "dy": (dy * (SEQUENCES * TOKENS) ** -0.5).astype(jnp.bfloat16)}
    for key, name in zip(kw, NAMES, strict=True):
        w = jax.random.normal(key, SHAPES[name], jnp.float32) * SHAPES[name][1] ** -0.5
        drawn[name] = (w * {"w_gate": 1.0, "w_up": bump(kh, FF, 4.0), "w_down": layers}[name]).astype(jnp.bfloat16)
    return drawn


def matmul(a, w):
    return jnp.dot(a, w, preferred_element_type=jnp.float32).astype(jnp.bfloat16)


def normed(h):
    wide = h.astype(jnp.float32)
    scale = lax.rsqrt(jnp.mean(wide**2, -1, keepdims=True) + 1e-6)
    return (wide * scale).astype(jnp.bfloat16)


def layer(h, w):
    a = normed(h)
    gate = jnp.dot(a, w["w_gate"], preferred_element_type=jnp.float32)
    up = jnp.dot(a, w["w_up"], preferred_element_type=jnp.float32)
    return h + matmul((jax.nn.silu(gate) * up).astype(jnp.bfloat16), w["w_down"])


def stack(weights, h):
    return lax.scan(lambda h, w: (layer(h, w), None), h, weights)[0]


def reference(x, dy, w_gate, w_up, w_down):
    weights = dict(zip(NAMES, (w_gate, w_up, w_down), strict=True))

    def take(so_far, sequence):
        h, by_y = sequence
        _, back = jax.vjp(stack, weights, h)
        by_weights, by_h = back(by_y)
        return jax.tree.map(lambda total, term: total + term.astype(jnp.float32), so_far, by_weights), by_h

    none_yet = {name: jnp.zeros(w.shape, jnp.float32) for name, w in weights.items()}
    by_weights, by_x = lax.scan(take, none_yet, (x, dy))
    return (by_x, *(by_weights[name].astype(jnp.bfloat16) for name in NAMES))
```

```python
import functools
import jax
import jax.numpy as jnp
from jax import lax
from jax.experimental import pallas as pl
from jax.experimental.pallas import tpu as pltpu
from jax.sharding import PartitionSpec as P

F32 = jnp.float32
BF16 = jnp.bfloat16
LAYERS, TOKENS, D, FF = 2, 2048, 768, 1792
GRID = (2, 2, 4, 2)
GU_UNITS = {"A": (0, 1), "B": (1, 1), "C": (2, 1)}
DN_UNITS = {"A": (0, 2), "B": (2, 3), "C": (5, 2)}
ALL = slice(None)


def place():
    me = lax.axis_index("dp")
    c = lax.rem(me, 2)
    z = lax.rem(me // 2, 4)
    y = lax.rem(me // 8, 2)
    x = me // 16
    return x, y, z, c


def index(x, y, z, c):
    return ((x * 2 + y) * 4 + z) * 2 + c


def after(z):
    return lax.rem(2 * z + 1, 5)


def before(z):
    return lax.rem(3 * z + 2, 5)


def greet():
    x, y, z, c = place()
    barrier = pltpu.get_barrier_semaphore()
    for other in (index(x, y, z, 1 - c), index(1 - x, y, z, c), index(x, 1 - y, z, c), index(x, y, after(z), c), index(x, y, before(z), c)):
        pl.semaphore_signal(barrier, inc=1, device_id={"dp": other}, device_id_type=pl.DeviceIdType.MESH)
    pl.semaphore_wait(barrier, 5)


class Copies:
    def __init__(self, send, recv):
        self.send, self.recv, self.made, self.used = send, recv, {}, 0

    def start(self, name, pairs, to):
        made = []
        for src, dst in pairs:
            copy = pltpu.make_async_remote_copy(src_ref=src, dst_ref=dst, send_sem=self.send.at[self.used], recv_sem=self.recv.at[self.used],
                                                device_id={"dp": to}, device_id_type=pl.DeviceIdType.MESH)
            copy.start()
            made.append(copy)
            self.used += 1
        assert name not in self.made
        self.made[name] = made

    def wait(self, name):
        for copy in self.made[name]:
            copy.wait_recv()

    def finish(self):
        for made in self.made.values():
            for copy in made:
                copy.wait_send()


GATHER_COPIES = 160


def gather_steps(copies, gu_in, dn_in, gu, dn, gs, ds, tag):
    x, y, z, c = place()
    X, Y = 1 - x, 1 - y
    ring = [z]
    for _ in range(3):
        ring.append(before(ring[-1]))
    to = {"x": index(X, y, z, c), "y": index(x, Y, z, c), "z": index(x, y, after(z), c), "c": index(x, y, z, 1 - c)}

    def region(colour, xs, ys, k):
        a, n = GU_UNITS[colour]
        b, m = DN_UNITS[colour]
        return (gu.at[gs, xs, ys, ring[k], c, pl.ds(a, n)], dn.at[ds, xs, ys, ring[k], c, pl.ds(b, m)])

    def own(colour):
        a, n = GU_UNITS[colour]
        b, m = DN_UNITS[colour]
        return (gu_in.at[gs, pl.ds(a, n)], dn_in.at[ds, pl.ds(b, m)])

    def send(name, way, colour, xs, ys, k, mine=False):
        dst = region(colour, xs, ys, k)
        src = own(colour) if mine else dst
        copies.start(tag + colour + name, tuple(zip(src, dst)), to[way])

    def arrived(name, colour, xs, ys, k):
        copies.wait(tag + colour + name)

    def share(name, colour, xs, ys, k):
        reg = region(colour, xs, ys, k)
        copies.start(tag + colour + name + "s", tuple(zip(reg, reg)), to["c"])
        shared.append((tag + colour + name + "s"))

    shared = []
    send("x", "x", "C", x, y, 0, True)
    send("y", "y", "B", x, y, 0, True)
    send("z1", "z", "A", x, y, 0, True)
    send("x0", "x", "A", x, y, 0, True)
    send("y0", "y", "A", x, y, 0, True)
    full = (gu.at[gs, x, y, z, c], dn.at[ds, x, y, z, c])
    copies.start(tag + "own", tuple(zip((gu_in.at[gs], dn_in.at[ds]), full)), to["c"])
    shared.append(tag + "own")
    yield
    yield
    copies.wait(tag + "Cx")
    send("z1", "z", "C", ALL, y, 0)
    send("y0", "y", "C", ALL, y, 0)
    share("x", "C", X, y, 0)
    yield
    copies.wait(tag + "By")
    send("z1", "z", "B", x, ALL, 0)
    send("x0", "x", "B", x, ALL, 0)
    share("y", "B", x, Y, 0)
    for k in (1, 2, 3):
        yield
        copies.wait(tag + f"Az{k}")
        if k < 3:
            send(f"z{k + 1}", "z", "A", x, y, k)
        send(f"x{k}", "x", "A", x, y, k)
        send(f"y{k}", "y", "A", x, y, k)
        share(f"z{k}", "A", x, y, k)
        yield
        copies.wait(tag + f"Ax{k - 1}")
        send(f"Y{k - 1}", "y", "A", X, y, k - 1)
        share(f"x{k - 1}", "A", X, y, k - 1)
        yield
        copies.wait(tag + f"Cz{k}")
        if k < 3:
            send(f"z{k + 1}", "z", "C", ALL, y, k)
        send(f"y{k}", "y", "C", ALL, y, k)
        share(f"z{k}", "C", ALL, y, k)
        yield
        copies.wait(tag + f"Bz{k}")
        if k < 3:
            send(f"z{k + 1}", "z", "B", x, ALL, k)
        send(f"x{k}", "x", "B", x, ALL, k)
        share(f"z{k}", "B", x, ALL, k)
    yield
    copies.wait(tag + "Ax3")
    send("Y3", "y", "A", X, y, 3)
    share("x3", "A", X, y, 3)
    for k in range(4):
        yield
        copies.wait(tag + f"Bx{k}")
        share(f"x{k}", "B", X, ALL, k)
        yield
        copies.wait(tag + f"Cy{k}")
        share(f"y{k}", "C", ALL, Y, k)
        yield
        copies.wait(tag + f"Ay{k}")
        copies.wait(tag + f"AY{k}")
        share(f"y{k}", "A", ALL, Y, k)
    for name in shared:
        yield
        copies.wait(name)


def gather_kernel(gu_in, dn_in, gu, dn, gu_own, dn_own, send, recv, local):
    x, y, z, c = place()
    greet()
    copies = Copies(send, recv)
    steps = gather_steps(copies, gu_in, dn_in, gu, dn, ALL, ALL, "")
    next(steps)
    one = pltpu.make_async_copy(gu_in, gu_own, local.at[0])
    two = pltpu.make_async_copy(dn_in, dn_own, local.at[1])
    one.start()
    two.start()
    one.wait()
    two.wait()
    one = pltpu.make_async_copy(gu_own, gu.at[ALL, x, y, z, c], local.at[2])
    two = pltpu.make_async_copy(dn_own, dn.at[ALL, x, y, z, c], local.at[3])
    one.start()
    two.start()
    one.wait()
    two.wait()
    for _ in steps:
        pass
    copies.finish()


def gather(gu_in, dn_in):
    hbm = pl.BlockSpec(memory_space=pl.ANY)
    return pl.pallas_call(
        gather_kernel, name="gather",
        out_shape=(jax.ShapeDtypeStruct((4, *GRID, 3, 8, FF), BF16), jax.ShapeDtypeStruct((2, *GRID, 7, 8, D), BF16)),
        in_specs=[hbm, hbm], out_specs=(hbm, hbm),
        scratch_shapes=[pltpu.VMEM((4, 3, 8, FF), BF16), pltpu.VMEM((2, 7, 8, D), BF16),
                        pltpu.SemaphoreType.DMA((GATHER_COPIES,)), pltpu.SemaphoreType.DMA((GATHER_COPIES,)), pltpu.SemaphoreType.DMA((4,))],
        compiler_params=pltpu.CompilerParams(collective_id=0, has_side_effects=True),
    )(gu_in, dn_in)


SCATTER_COPIES = 700
ROOM = 15


def add_pairs(dst, src, count, pairs):
    def body(m, _):
        for i, j in pairs:
            dst[(m, *i)] = (dst[(m, *i)].astype(F32) + src[(m, *j)].astype(F32)).astype(BF16)
        return 0
    lax.fori_loop(0, count, body, 0)


def scatter_steps(copies, gus, dns, gu, dn, sgu, sdn, arrive, tag):
    x, y, z, c = place()
    X, Y = 1 - x, 1 - y
    ring = [z]
    for _ in range(3):
        ring.append(before(ring[-1]))
    to = {"x": index(X, y, z, c), "y": index(x, Y, z, c), "z": index(x, y, after(z), c), "c": index(x, y, z, 1 - c)}
    M, N = len(gus), len(dns)
    slots, used = {}, {"A": 0, "B": 0, "C": 0}

    def half(colour, far):
        if colour == "B":
            return (X if far else x), ALL
        return ALL, (Y if far else y)

    def blocks(xs, ys):
        return [(e, ys) for e in range(2)] if xs is ALL else [(xs, e) for e in range(2)] if ys is ALL else [(xs, ys)]

    def swap(k, far):
        for colour in "ACB":
            xs, ys = half(colour, far)
            (a, n), (b, m) = GU_UNITS[colour], DN_UNITS[colour]
            pairs = [(gus[i].at[xs, ys, ring[k], 1 - c, pl.ds(a, n)], sgu.at[i, xs, ys, ring[k], pl.ds(a, n)]) for i in range(M)]
            pairs += [(dns[i].at[xs, ys, ring[k], 1 - c, pl.ds(b, m)], sdn.at[i, xs, ys, ring[k], pl.ds(b, m)]) for i in range(N)]
            copies.start(f"{tag}s{colour}{k}{far}", pairs, to["c"])

    def swapped(k, far):
        for colour in "ACB":
            copies.wait(f"{tag}s{colour}{k}{far}")
            here = blocks(*half(colour, far))
            for buf, other, count, (a, n) in ((gu, sgu, M, GU_UNITS[colour]), (dn, sdn, N, DN_UNITS[colour])):
                at = [(bx, by, ring[k], a + u) for bx, by in here for u in range(n)]
                add_pairs(buf, other, count, [(i, i) for i in at])

    def send(name, way, colour, xs, ys, k):
        (a, n), (b, m) = GU_UNITS[colour], DN_UNITS[colour]
        number = len(blocks(xs, ys))
        at = used[colour]
        used[colour] += number
        slots[colour + name] = at
        to_at = pl.ds(at, number) if number == 2 else at
        rgu, rdn = arrive[colour]
        copies.start(tag + colour + name, [(gu.at[ALL, xs, ys, ring[k], pl.ds(a, n)], rgu.at[ALL, to_at]),
                                           (dn.at[ALL, xs, ys, ring[k], pl.ds(b, m)], rdn.at[ALL, to_at])], to[way])

    def take(name, colour, xs, ys, k):
        copies.wait(tag + colour + name)
        at = slots[colour + name]
        for buf, other, count, (a, n) in ((gu, arrive[colour][0], M, GU_UNITS[colour]), (dn, arrive[colour][1], N, DN_UNITS[colour])):
            pairs = [((bx, by, ring[k], a + u), (at + e, u)) for e, (bx, by) in enumerate(blocks(xs, ys)) for u in range(n)]
            add_pairs(buf, other, count, pairs)

    def far(k):
        swapped(k, True)
        send(f"y{k}", "y", "A", ALL, Y, k)
        send(f"y{k}", "y", "C", ALL, Y, k)
        send(f"x{k}", "x", "B", X, ALL, k)

    def second(k):
        t = k or 4
        take(f"y{k}", "A", ALL, y, k)
        send(f"x{k}", "x", "A", X, y, k)
        yield
        take(f"y{k}", "C", ALL, y, k)
        if t > 1:
            take(f"z{t - 1}", "C", ALL, y, k)
        if t < 4:
            send(f"z{t}", "z", "C", ALL, y, k)
        else:
            send("x", "x", "C", X, y, k)
        yield
        take(f"x{k}", "B", x, ALL, k)
        if t > 1:
            take(f"z{t - 1}", "B", x, ALL, k)
        if t < 4:
            send(f"z{t}", "z", "B", x, ALL, k)
        else:
            send("y", "y", "B", x, Y, k)

    def third(k):
        t = k or 4
        take(f"x{k}", "A", x, y, k)
        if t > 1:
            take(f"z{t - 1}", "A", x, y, k)
        if t < 4:
            send(f"z{t}", "z", "A", x, y, k)

    for k, away in ((1, True), (2, True), (1, False), (3, True), (2, False), (0, True), (3, False), (0, False)):
        swap(k, away)
    yield
    far(1)
    yield
    far(2)
    yield
    swapped(1, False)
    yield
    yield from second(1)
    yield
    far(3)
    yield
    swapped(2, False)
    yield
    third(1)
    yield
    yield from second(2)
    yield
    far(0)
    yield
    swapped(3, False)
    yield
    third(2)
    yield
    yield from second(3)
    yield
    swapped(0, False)
    yield
    third(3)
    yield
    yield from second(0)
    yield
    third(0)
    yield
    take("x", "C", x, y, 0)
    yield
    take("y", "B", x, y, 0)


def scatter_scratch(M, N):
    return ([pltpu.VMEM((M, 2, 2, 4, 3, 8, FF), BF16), pltpu.VMEM((N, 2, 2, 4, 7, 8, D), BF16)] * 2
            + [pltpu.VMEM((M, ROOM, GU_UNITS[o][1], 8, FF), BF16) for o in "ABC"] + [pltpu.VMEM((N, ROOM, DN_UNITS[o][1], 8, D), BF16) for o in "ABC"])


def scatter_kernel(M, N, *refs):
    gus, dns = refs[:M], refs[M:M + N]
    gu_out, dn_out = refs[M + N:M + N + 2]
    gu, dn, sgu, sdn, ga, gb, gc, da, db, dc, send, recv, local = refs[M + N + 2:]
    x, y, z, c = place()
    greet()
    copies = Copies(send, recv)
    steps = scatter_steps(copies, gus, dns, gu, dn, sgu, sdn, {"A": (ga, da), "B": (gb, db), "C": (gc, dc)}, "")
    next(steps)
    loads = [pltpu.make_async_copy(gus[i].at[ALL, ALL, ALL, c], gu.at[i], local.at[i]) for i in range(M)]
    loads += [pltpu.make_async_copy(dns[i].at[ALL, ALL, ALL, c], dn.at[i], local.at[M + i]) for i in range(N)]
    for load in loads:
        load.start()
    for load in loads:
        load.wait()
    for _ in steps:
        pass
    stores = [pltpu.make_async_copy(gu.at[ALL, x, y, z], gu_out, local.at[0]), pltpu.make_async_copy(dn.at[ALL, x, y, z], dn_out, local.at[1])]
    for store in stores:
        store.start()
    for store in stores:
        store.wait()
    copies.finish()


def scatter(gus, dns, number=1):
    M, N = len(gus), len(dns)
    hbm = pl.BlockSpec(memory_space=pl.ANY)
    return pl.pallas_call(
        functools.partial(scatter_kernel, M, N), name="scatter",
        out_shape=(jax.ShapeDtypeStruct((M, 3, 8, FF), BF16), jax.ShapeDtypeStruct((N, 7, 8, D), BF16)),
        in_specs=[hbm] * (M + N), out_specs=(hbm, hbm),
        scratch_shapes=[*scatter_scratch(M, N), pltpu.SemaphoreType.DMA((SCATTER_COPIES,)), pltpu.SemaphoreType.DMA((SCATTER_COPIES,)), pltpu.SemaphoreType.DMA((M + N,))],
        compiler_params=pltpu.CompilerParams(collective_id=number, has_side_effects=True, vmem_limit_bytes=60 * 1024 * 1024),
    )(*gus, *dns)


def dot(a, b, ca, cb):
    return lax.dot_general(a, b, (((ca,), (cb,)), ((), ())), preferred_element_type=F32)


def compute(x, dy, wg, wu, wd):
    saved = []
    h = x
    for l in range(LAYERS):
        wide = h.astype(F32)
        s = lax.rsqrt(jnp.mean(wide**2, -1, keepdims=True) + 1e-6)
        a = (wide * s).astype(BF16)
        g, u = dot(a, wg[l], 1, 0), dot(a, wu[l], 1, 0)
        p = (jax.nn.silu(g) * u).astype(BF16)
        saved.append((h, s, a, g, u, p))
        if l < LAYERS - 1:
            h = h + dot(p, wd[l], 1, 0).astype(BF16)
    ct, grads = dy, [None] * LAYERS
    for l in reversed(range(LAYERS)):
        h, s, a, g, u, p = saved[l]
        by_down = dot(p, ct, 0, 0).astype(BF16)
        by_p = dot(ct, wd[l], 1, 1).astype(BF16).astype(F32)
        sig = jax.nn.sigmoid(g)
        by_u = (by_p * g * sig).astype(BF16)
        by_g = (by_p * u * (sig * (1 + g * (1 - sig)))).astype(BF16)
        by_gate, by_up = dot(a, by_g, 0, 0).astype(BF16), dot(a, by_u, 0, 0).astype(BF16)
        by_a = dot(by_g, wg[l], 1, 1) + dot(by_u, wu[l], 1, 1)
        n = h.astype(F32) * s
        ct = (ct.astype(F32) + s * (by_a - n * jnp.mean(by_a * n, -1, keepdims=True))).astype(BF16)
        grads[l] = (by_gate, by_up, by_down)
    return ct, grads


def solution(mesh):
    def step(x, dy, w_gate, w_up, w_down):
        gu_in = jnp.concatenate([w_gate, w_up]).reshape(4, 3, 8, FF)
        gu, dn = gather(gu_in, w_down.reshape(2, 7, 8, D))
        gu, dn = gu.reshape(4, D, FF), dn.reshape(2, FF, D)
        ct, grads = compute(x[0], dy[0], gu[:2], gu[2:], dn)
        gus = [grads[l][i].reshape(*GRID, 3, 8, FF) for i in (0, 1) for l in (0, 1)]
        dns = [grads[l][2].reshape(*GRID, 7, 8, D) for l in (0, 1)]
        by_gu, by_dn = scatter(gus, dns)
        by_gu = by_gu.reshape(4, 24, FF)
        return ct[None], by_gu[:2], by_gu[2:], by_dn.reshape(2, 56, D)

    rows = P(None, "dp", None)
    tokens = P(("rep", "dp"), None, None)
    return jax.shard_map(step, mesh=mesh, in_specs=(tokens, tokens, rows, rows, rows), out_specs=(tokens, P("rep", "dp", None), P("rep", "dp", None), P("rep", "dp", None)), check_vma=False)
```

```python
import functools
import jax
import jax.numpy as jnp
from jax import lax
from jax.experimental import pallas as pl
from jax.experimental.pallas import tpu as pltpu
from jax.sharding import PartitionSpec as P

F32 = jnp.float32
BF16 = jnp.bfloat16
LAYERS, TOKENS, D, FF = 2, 2048, 768, 1792
GRID = (2, 2, 4, 2)
GU_UNITS = {"A": (0, 1), "B": (1, 1), "C": (2, 1)}
DN_UNITS = {"A": (0, 2), "B": (2, 3), "C": (5, 2)}
ALL = slice(None)


def place():
    me = lax.axis_index("dp")
    c = lax.rem(me, 2)
    z = lax.rem(me // 2, 4)
    y = lax.rem(me // 8, 2)
    x = me // 16
    return x, y, z, c


def index(x, y, z, c):
    return ((x * 2 + y) * 4 + z) * 2 + c


def after(z):
    return lax.rem(2 * z + 1, 5)


def before(z):
    return lax.rem(3 * z + 2, 5)


def greet():
    x, y, z, c = place()
    barrier = pltpu.get_barrier_semaphore()
    for other in (index(x, y, z, 1 - c), index(1 - x, y, z, c), index(x, 1 - y, z, c), index(x, y, after(z), c), index(x, y, before(z), c)):
        pl.semaphore_signal(barrier, inc=1, device_id={"dp": other}, device_id_type=pl.DeviceIdType.MESH)
    pl.semaphore_wait(barrier, 5)


class Copies:
    def __init__(self, send, recv):
        self.send, self.recv, self.made, self.used = send, recv, {}, 0

    def group(self, name):
        first, pairs, to = self.made[name]
        return [pltpu.make_async_remote_copy(src_ref=src, dst_ref=dst, send_sem=self.send.at[first + i], recv_sem=self.recv.at[first + i],
                                             device_id={"dp": to}, device_id_type=pl.DeviceIdType.MESH) for i, (src, dst) in enumerate(pairs())]

    def start(self, name, pairs, to):
        assert name not in self.made
        self.made[name] = (self.used, pairs, to)
        for copy in self.group(name):
            copy.start()
            self.used += 1

    def wait(self, name):
        for copy in self.group(name):
            copy.wait_recv()

    def finish(self):
        for name in self.made:
            for copy in self.group(name):
                copy.wait_send()


GATHER_COPIES = 160


def gather_steps(copies, gu_in, dn_in, gu, dn, gs, ds, tag):
    x, y, z, c = place()
    X, Y = 1 - x, 1 - y
    ring = [z]
    for _ in range(3):
        ring.append(before(ring[-1]))
    to = {"x": index(X, y, z, c), "y": index(x, Y, z, c), "z": index(x, y, after(z), c), "c": index(x, y, z, 1 - c)}

    def region(colour, xs, ys, k):
        a, n = GU_UNITS[colour]
        b, m = DN_UNITS[colour]
        return (gu.at[gs, xs, ys, ring[k], c, pl.ds(a, n)], dn.at[ds, xs, ys, ring[k], c, pl.ds(b, m)])

    def own(colour):
        a, n = GU_UNITS[colour]
        b, m = DN_UNITS[colour]
        return (gu_in.at[gs, pl.ds(a, n)], dn_in.at[ds, pl.ds(b, m)])

    def send(name, way, colour, xs, ys, k, mine=False):
        def pairs():
            dst = region(colour, xs, ys, k)
            return list(zip(own(colour) if mine else dst, dst))
        copies.start(tag + colour + name, pairs, to[way])

    def arrived(name, colour, xs, ys, k):
        copies.wait(tag + colour + name)

    def share(name, colour, xs, ys, k):
        def pairs():
            reg = region(colour, xs, ys, k)
            return list(zip(reg, reg))
        copies.start(tag + colour + name + "s", pairs, to["c"])
        shared.append((tag + colour + name + "s"))

    shared = []
    send("x", "x", "C", x, y, 0, True)
    send("y", "y", "B", x, y, 0, True)
    send("z1", "z", "A", x, y, 0, True)
    send("x0", "x", "A", x, y, 0, True)
    send("y0", "y", "A", x, y, 0, True)
    copies.start(tag + "own", lambda: [(gu_in.at[gs], gu.at[gs, x, y, z, c]), (dn_in.at[ds], dn.at[ds, x, y, z, c])], to["c"])
    shared.append(tag + "own")
    yield
    yield
    copies.wait(tag + "Cx")
    send("z1", "z", "C", ALL, y, 0)
    send("y0", "y", "C", ALL, y, 0)
    share("x", "C", X, y, 0)
    yield
    copies.wait(tag + "By")
    send("z1", "z", "B", x, ALL, 0)
    send("x0", "x", "B", x, ALL, 0)
    share("y", "B", x, Y, 0)
    for k in (1, 2, 3):
        yield
        copies.wait(tag + f"Az{k}")
        if k < 3:
            send(f"z{k + 1}", "z", "A", x, y, k)
        send(f"x{k}", "x", "A", x, y, k)
        send(f"y{k}", "y", "A", x, y, k)
        share(f"z{k}", "A", x, y, k)
        yield
        copies.wait(tag + f"Ax{k - 1}")
        send(f"Y{k - 1}", "y", "A", X, y, k - 1)
        share(f"x{k - 1}", "A", X, y, k - 1)
        yield
        copies.wait(tag + f"Cz{k}")
        if k < 3:
            send(f"z{k + 1}", "z", "C", ALL, y, k)
        send(f"y{k}", "y", "C", ALL, y, k)
        share(f"z{k}", "C", ALL, y, k)
        yield
        copies.wait(tag + f"Bz{k}")
        if k < 3:
            send(f"z{k + 1}", "z", "B", x, ALL, k)
        send(f"x{k}", "x", "B", x, ALL, k)
        share(f"z{k}", "B", x, ALL, k)
    yield
    copies.wait(tag + "Ax3")
    send("Y3", "y", "A", X, y, 3)
    share("x3", "A", X, y, 3)
    for k in range(4):
        yield
        copies.wait(tag + f"Bx{k}")
        share(f"x{k}", "B", X, ALL, k)
        yield
        copies.wait(tag + f"Cy{k}")
        share(f"y{k}", "C", ALL, Y, k)
        yield
        copies.wait(tag + f"Ay{k}")
        copies.wait(tag + f"AY{k}")
        share(f"y{k}", "A", ALL, Y, k)
    for name in shared:
        yield
        copies.wait(name)


def gather_kernel(gu_in, dn_in, gu, dn, gu_own, dn_own, send, recv, local):
    x, y, z, c = place()
    greet()
    copies = Copies(send, recv)
    steps = gather_steps(copies, gu_in, dn_in, gu, dn, ALL, ALL, "")
    next(steps)
    one = pltpu.make_async_copy(gu_in, gu_own, local.at[0])
    two = pltpu.make_async_copy(dn_in, dn_own, local.at[1])
    one.start()
    two.start()
    one.wait()
    two.wait()
    one = pltpu.make_async_copy(gu_own, gu.at[ALL, x, y, z, c], local.at[2])
    two = pltpu.make_async_copy(dn_own, dn.at[ALL, x, y, z, c], local.at[3])
    one.start()
    two.start()
    one.wait()
    two.wait()
    for _ in steps:
        pass
    copies.finish()


def gather(gu_in, dn_in):
    hbm = pl.BlockSpec(memory_space=pl.ANY)
    return pl.pallas_call(
        gather_kernel, name="gather",
        out_shape=(jax.ShapeDtypeStruct((4, *GRID, 3, 8, FF), BF16), jax.ShapeDtypeStruct((2, *GRID, 7, 8, D), BF16)),
        in_specs=[hbm, hbm], out_specs=(hbm, hbm),
        scratch_shapes=[pltpu.VMEM((4, 3, 8, FF), BF16), pltpu.VMEM((2, 7, 8, D), BF16),
                        pltpu.SemaphoreType.DMA((GATHER_COPIES,)), pltpu.SemaphoreType.DMA((GATHER_COPIES,)), pltpu.SemaphoreType.DMA((4,))],
        compiler_params=pltpu.CompilerParams(collective_id=0, has_side_effects=True),
    )(gu_in, dn_in)


SCATTER_COPIES = 300
ROOM = 15


def add_pairs(dst, src, count, pairs):
    def body(m, _):
        for i, j in pairs:
            dst[(m, *i)] = (dst[(m, *i)].astype(F32) + src[(m, *j)].astype(F32)).astype(BF16)
        return 0
    lax.fori_loop(0, count, body, 0)


def scatter_steps(copies, M, N, gus, dns, gu, dn, sgu, sdn, arrive, tag):
    x, y, z, c = place()
    X, Y = 1 - x, 1 - y
    ring = [z]
    for _ in range(3):
        ring.append(before(ring[-1]))
    to = {"x": index(X, y, z, c), "y": index(x, Y, z, c), "z": index(x, y, after(z), c), "c": index(x, y, z, 1 - c)}
    other = 1 - c
    slots, used = {}, {"A": 0, "B": 0, "C": 0}

    def half(colour, far):
        if colour == "B":
            return (X if far else x), ALL
        return ALL, (Y if far else y)

    def blocks(xs, ys):
        return [(e, ys) for e in range(2)] if xs is ALL else [(xs, e) for e in range(2)] if ys is ALL else [(xs, ys)]

    def swap(k, far):
        for colour in "ACB":
            xs, ys = half(colour, far)
            (a, n), (b, m) = GU_UNITS[colour], DN_UNITS[colour]

            def pairs(xs=xs, ys=ys, a=a, n=n, b=b, m=m):
                return ([(gus(i).at[xs, ys, ring[k], other, pl.ds(a, n)], sgu.at[i, xs, ys, ring[k], pl.ds(a, n)]) for i in range(M)]
                        + [(dns(i).at[xs, ys, ring[k], other, pl.ds(b, m)], sdn.at[i, xs, ys, ring[k], pl.ds(b, m)]) for i in range(N)])
            copies.start(f"{tag}s{colour}{k}{far}", pairs, to["c"])

    def swapped(k, far):
        for colour in "ACB":
            copies.wait(f"{tag}s{colour}{k}{far}")
            here = blocks(*half(colour, far))
            for buf, other, count, (a, n) in ((gu, sgu, M, GU_UNITS[colour]), (dn, sdn, N, DN_UNITS[colour])):
                at = [(bx, by, ring[k], a + u) for bx, by in here for u in range(n)]
                add_pairs(buf, other, count, [(i, i) for i in at])

    def send(name, way, colour, xs, ys, k):
        (a, n), (b, m) = GU_UNITS[colour], DN_UNITS[colour]
        number = len(blocks(xs, ys))
        at = used[colour]
        used[colour] += number
        slots[colour + name] = at
        rgu, rdn = arrive[colour]

        def pairs():
            to_at = pl.ds(at, number) if number == 2 else at
            return [(gu.at[ALL, xs, ys, ring[k], pl.ds(a, n)], rgu.at[ALL, to_at]), (dn.at[ALL, xs, ys, ring[k], pl.ds(b, m)], rdn.at[ALL, to_at])]
        copies.start(tag + colour + name, pairs, to[way])

    def take(name, colour, xs, ys, k):
        copies.wait(tag + colour + name)
        at = slots[colour + name]
        for buf, other, count, (a, n) in ((gu, arrive[colour][0], M, GU_UNITS[colour]), (dn, arrive[colour][1], N, DN_UNITS[colour])):
            pairs = [((bx, by, ring[k], a + u), (at + e, u)) for e, (bx, by) in enumerate(blocks(xs, ys)) for u in range(n)]
            add_pairs(buf, other, count, pairs)

    def far(k):
        swapped(k, True)
        send(f"y{k}", "y", "A", ALL, Y, k)
        send(f"y{k}", "y", "C", ALL, Y, k)
        send(f"x{k}", "x", "B", X, ALL, k)

    def second(k):
        t = k or 4
        take(f"y{k}", "A", ALL, y, k)
        send(f"x{k}", "x", "A", X, y, k)
        yield
        take(f"y{k}", "C", ALL, y, k)
        if t > 1:
            take(f"z{t - 1}", "C", ALL, y, k)
        if t < 4:
            send(f"z{t}", "z", "C", ALL, y, k)
        else:
            send("x", "x", "C", X, y, k)
        yield
        take(f"x{k}", "B", x, ALL, k)
        if t > 1:
            take(f"z{t - 1}", "B", x, ALL, k)
        if t < 4:
            send(f"z{t}", "z", "B", x, ALL, k)
        else:
            send("y", "y", "B", x, Y, k)

    def third(k):
        t = k or 4
        take(f"x{k}", "A", x, y, k)
        if t > 1:
            take(f"z{t - 1}", "A", x, y, k)
        if t < 4:
            send(f"z{t}", "z", "A", x, y, k)

    yield
    for k, away in ((1, True), (2, True), (1, False), (3, True), (2, False), (0, True), (3, False), (0, False)):
        swap(k, away)
    yield
    far(1)
    yield
    far(2)
    yield
    swapped(1, False)
    yield
    yield from second(1)
    yield
    far(3)
    yield
    swapped(2, False)
    yield
    third(1)
    yield
    yield from second(2)
    yield
    far(0)
    yield
    swapped(3, False)
    yield
    third(2)
    yield
    yield from second(3)
    yield
    swapped(0, False)
    yield
    third(3)
    yield
    yield from second(0)
    yield
    third(0)
    yield
    take("x", "C", x, y, 0)
    yield
    take("y", "B", x, y, 0)


def scatter_scratch(M, N):
    return ([pltpu.VMEM((M, 2, 2, 4, 3, 8, FF), BF16), pltpu.VMEM((N, 2, 2, 4, 7, 8, D), BF16)] * 2
            + [pltpu.VMEM((M, ROOM, GU_UNITS[o][1], 8, FF), BF16) for o in "ABC"] + [pltpu.VMEM((N, ROOM, DN_UNITS[o][1], 8, D), BF16) for o in "ABC"])


TILE, CHUNK = 256, 512
TILES, CHUNKS = FF // TILE, TOKENS // CHUNK
MIB = 1024 * 1024


def dot(a, b, ca, cb):
    return lax.dot_general(a, b, (((ca,), (cb,)), ((), ())), preferred_element_type=F32)


def back_kernel(dy, h0, h1, wgu, wd, g0, u0, g1, u1, dx, gu_out, dn_out, gus, dns, *scratch):
    (ct, hbuf, at, acc, gate, up, wgu_t, wd_t, p, dgu, stage, stage_dn,
     gu1, dn1, sgu1, sdn1, ga1, gb1, gc1, da1, db1, dc1, gu0_, dn0_, sgu0, sdn0, ga0, gb0, gc0, da0, db0, dc0,
     send1, recv1, send0, recv0, sem_in, sem_h, sem_out, sem_own) = scratch
    x, y, z, c = place()
    greet()

    def terms(l, i):
        return gus.at[2 * i + l].reshape(*GRID, 3, 8, FF)

    def terms_dn(l, i):
        return dns.at[l].reshape(*GRID, 7, 8, D)

    runs = {}
    for l, (gu, dn, sgu, sdn, arrive, send, recv) in {
        1: (gu1, dn1, sgu1, sdn1, {"A": (ga1, da1), "B": (gb1, db1), "C": (gc1, dc1)}, send1, recv1),
        0: (gu0_, dn0_, sgu0, sdn0, {"A": (ga0, da0), "B": (gb0, db0), "C": (gc0, dc0)}, send0, recv0),
    }.items():
        copies = Copies(send, recv)
        steps = scatter_steps(copies, 2, 1, functools.partial(terms, l), functools.partial(terms_dn, l), gu, dn, sgu, sdn, arrive, "")
        next(steps)

        def loads(l=l, gu=gu, dn=dn):
            return ([pltpu.make_async_copy(terms(l, i).at[ALL, ALL, ALL, c], gu.at[i], sem_own.at[l, i]) for i in range(2)]
                    + [pltpu.make_async_copy(terms_dn(l, 0).at[ALL, ALL, ALL, c], dn.at[0], sem_own.at[l, 2])])
        runs[l] = (copies, steps, loads, gu, dn)

    def begin(l):
        copies, steps, loads, _, _ = runs[l]
        for load in loads():
            load.start()
        next(steps)

    def arrived(l):
        for load in runs[l][2]():
            load.wait()

    def go(l, number):
        for _ in range(number):
            next(runs[l][1], None)

    def inputs(step, slot, act):
        l, f = 1 - step // TILES, lax.rem(step, TILES)
        cols = pl.ds(pl.multiple_of(f * TILE, TILE), TILE)
        copies = [(wgu.at[l, :, cols], wgu_t.at[slot, :, pl.ds(0, TILE)]), (wgu.at[2 + l, :, cols], wgu_t.at[slot, :, pl.ds(TILE, TILE)]), (wd.at[l, cols, :], wd_t.at[slot])]
        for i, (src, dst) in enumerate(copies):
            act(pltpu.make_async_copy(src, dst, sem_in.at[slot, i]))
        for number, (gs, us) in ((1, (g1, u1)), (0, (g0, u0))):
            @pl.when(l == number)
            def _():
                act(pltpu.make_async_copy(gs.at[:, cols], gate.at[slot], sem_in.at[slot, 3]))
                act(pltpu.make_async_copy(us.at[:, cols], up.at[slot], sem_in.at[slot, 4]))

    def outputs(step, act):
        l, f = 1 - step // TILES, lax.rem(step, TILES)
        cols = pl.ds(pl.multiple_of(f * TILE, TILE), TILE)
        act(pltpu.make_async_copy(stage.at[:, pl.ds(0, TILE)], gus.at[l, :, cols], sem_out.at[0]))
        act(pltpu.make_async_copy(stage.at[:, pl.ds(TILE, TILE)], gus.at[2 + l, :, cols], sem_out.at[1]))
        act(pltpu.make_async_copy(stage_dn, dns.at[l, cols, :], sem_out.at[2]))

    start, wait = (lambda copy: copy.start()), (lambda copy: copy.wait())
    first = pltpu.make_async_copy(dy, ct, sem_h.at[0])
    states = pltpu.make_async_copy(h1, hbuf, sem_h.at[1])
    first.start()
    states.start()
    inputs(0, 0, start)
    first.wait()

    def body(step, _):
        l, f, slot = 1 - step // TILES, lax.rem(step, TILES), lax.rem(step, 2)
        inputs(step, slot, wait)

        @pl.when(step + 1 < 2 * TILES)
        def _():
            inputs(step + 1, 1 - slot, start)

        @pl.when(f == 0)
        def _():
            pltpu.make_async_copy(h1, hbuf, sem_h.at[1]).wait()

            def norm(t, _):
                rows = pl.ds(pl.multiple_of(t * 256, 256), 256)
                wide = hbuf[rows, :].astype(F32)
                n = wide * lax.rsqrt(jnp.mean(wide * wide, -1, keepdims=True) + 1e-6)
                at[:, rows] = n.T.astype(BF16)
                acc[rows, :] = jnp.zeros((256, D), F32)
                return 0
            lax.fori_loop(0, TOKENS // 256, norm, 0)

        def hidden(t, _):
            rows = pl.ds(pl.multiple_of(t * CHUNK, CHUNK), CHUNK)
            by_p = dot(ct[rows, :], wd_t[slot], 1, 1).astype(BF16).astype(F32)
            g, u = gate[slot, rows, :], up[slot, rows, :]
            sig = 1.0 / (1.0 + jnp.exp(-g))
            silu = g * sig
            p[rows, :] = (silu * u).astype(BF16)
            dgu[rows, pl.ds(TILE, TILE)] = (by_p * silu).astype(BF16)
            dgu[rows, pl.ds(0, TILE)] = (by_p * u * (sig * (1.0 + g * (1.0 - sig)))).astype(BF16)
            return 0
        lax.fori_loop(0, CHUNKS, hidden, 0)

        @pl.when(f > 0)
        def _():
            outputs(step - 1, wait)
        stage_dn[...] = dot(p[...], ct[...], 0, 0).astype(BF16)

        def weights(r, _):
            rows = pl.ds(pl.multiple_of(r * 256, 256), 256)
            stage[rows, :] = dot(at[rows, :], dgu[...], 1, 0).astype(BF16)
            return 0
        lax.fori_loop(0, D // 256, weights, 0)
        outputs(step, start)

        def states_back(t, _):
            rows = pl.ds(pl.multiple_of(t * CHUNK, CHUNK), CHUNK)
            acc[rows, :] += dot(dgu[rows, :], wgu_t[slot], 1, 1)
            return 0
        lax.fori_loop(0, CHUNKS, states_back, 0)

        @pl.when(f == TILES - 1)
        def _():
            outputs(step, wait)

            @pl.when(l == 1)
            def _():
                begin(1)

            @pl.when(l == 0)
            def _():
                begin(0)

            def norm_back(t, _):
                rows = pl.ds(pl.multiple_of(t * 256, 256), 256)
                wide = hbuf[rows, :].astype(F32)
                s = lax.rsqrt(jnp.mean(wide * wide, -1, keepdims=True) + 1e-6)
                n, by_a = wide * s, acc[rows, :]
                by_h = s * (by_a - n * jnp.mean(by_a * n, -1, keepdims=True))
                ct[rows, :] = (ct[rows, :].astype(F32) + by_h).astype(BF16)
                return 0
            lax.fori_loop(0, TOKENS // 256, norm_back, 0)

            @pl.when(l == 1)
            def _():
                pltpu.make_async_copy(h0, hbuf, sem_h.at[1]).start()
                arrived(1)

        for i in range(TILES):
            @pl.when(step == TILES + i)
            def _():
                go(1, EVENTS[i])
        return 0

    lax.fori_loop(0, 2 * TILES, body, 0)
    last = pltpu.make_async_copy(ct, dx, sem_h.at[0])
    last.start()
    arrived(0)
    go(1, 1000)
    go(0, 1000)
    ends = []
    for l in (1, 0):
        copies, _, _, gu, dn = runs[l]
        for i in range(2):
            ends.append(pltpu.make_async_copy(gu.at[i, x, y, z], gu_out.at[2 * i + l], sem_own.at[l, i]))
        ends.append(pltpu.make_async_copy(dn.at[0, x, y, z], dn_out.at[l], sem_own.at[l, 2]))
    for end in ends:
        end.start()
    for end in ends:
        end.wait()
    last.wait()
    runs[1][0].finish()
    runs[0][0].finish()


EVENTS = (5, 5, 5, 5, 5, 5, 5)


def back(dy, h0, h1, wgu, wd, g0, u0, g1, u1):
    hbm = pl.BlockSpec(memory_space=pl.ANY)
    vmem, dma = pltpu.VMEM, pltpu.SemaphoreType.DMA
    out = pl.pallas_call(
        back_kernel, name="back",
        out_shape=(jax.ShapeDtypeStruct((TOKENS, D), BF16), jax.ShapeDtypeStruct((4, 3, 8, FF), BF16), jax.ShapeDtypeStruct((2, 7, 8, D), BF16),
                   jax.ShapeDtypeStruct((4, D, FF), BF16), jax.ShapeDtypeStruct((2, FF, D), BF16)),
        in_specs=[hbm] * 9, out_specs=(hbm,) * 5,
        scratch_shapes=[vmem((TOKENS, D), BF16), vmem((TOKENS, D), BF16), vmem((D, TOKENS), BF16), vmem((TOKENS, D), F32),
                        vmem((2, TOKENS, TILE), F32), vmem((2, TOKENS, TILE), F32), vmem((2, D, 2 * TILE), BF16), vmem((2, TILE, D), BF16),
                        vmem((TOKENS, TILE), BF16), vmem((TOKENS, 2 * TILE), BF16), vmem((D, 2 * TILE), BF16), vmem((TILE, D), BF16),
                        *scatter_scratch(2, 1), *scatter_scratch(2, 1),
                        *[dma((SCATTER_COPIES,))] * 4, dma((2, 5)), dma((2,)), dma((3,)), dma((2, 3))],
        compiler_params=pltpu.CompilerParams(collective_id=1, has_side_effects=True, vmem_limit_bytes=63 * MIB),
    )(dy, h0, h1, wgu, wd, g0, u0, g1, u1)
    return out[:3]


def normed(h):
    wide = h.astype(F32)
    return (wide * lax.rsqrt(jnp.mean(wide**2, -1, keepdims=True) + 1e-6)).astype(BF16)


def solution(mesh):
    def step(x, dy, w_gate, w_up, w_down):
        gu_in = jnp.concatenate([w_gate, w_up]).reshape(4, 3, 8, FF)
        gu, dn = gather(gu_in, w_down.reshape(2, 7, 8, D))
        gu, dn = gu.reshape(4, D, FF), dn.reshape(2, FF, D)
        x, dy = x[0], dy[0]
        a = normed(x)
        g0, u0 = dot(a, gu[0], 1, 0), dot(a, gu[2], 1, 0)
        h = x + dot((jax.nn.silu(g0) * u0).astype(BF16), dn[0], 1, 0).astype(BF16)
        a = normed(h)
        g1, u1 = dot(a, gu[1], 1, 0), dot(a, gu[3], 1, 0)
        dx, by_gu, by_dn = back(dy, x, h, gu, dn, g0, u0, g1, u1)
        by_gu = by_gu.reshape(4, 24, FF)
        return dx[None], by_gu[:2], by_gu[2:], by_dn.reshape(2, 56, D)

    rows = P(None, "dp", None)
    tokens = P(("rep", "dp"), None, None)
    return jax.shard_map(step, mesh=mesh, in_specs=(tokens, tokens, rows, rows, rows), out_specs=(tokens, P("rep", "dp", None), P("rep", "dp", None), P("rep", "dp", None)), check_vma=False)
```

```python
import jax
import jax.numpy as jnp
from jax import lax
from jax.experimental import pallas as pl
from jax.experimental.pallas import tpu as pltpu
from jax.sharding import PartitionSpec as P

F32 = jnp.float32
BF16 = jnp.bfloat16
LAYERS, TOKENS, D, FF = 2, 2048, 768, 1792
NX, NY, NZ, NC = GRID = (2, 2, 4, 2)
ROWS = 8
GU_UNITS = {"A": (0, 1), "C": (1, 1), "B": (2, 1), "AC": (0, 2), "all": 3}
DN_UNITS = {"A": (0, 2), "C": (2, 2), "B": (4, 3), "AC": (0, 4), "all": 7}
ALL = slice(None)
YES, NO = True, False
MESH = pl.DeviceIdType.MESH
CHIPS = NX * NY * NZ
ARRIVALS = CHIPS - 1
TILE = 256
TILES = FF // TILE
EPS = 1e-6
LIMIT = 63 * 2**20


def place():
    me = lax.axis_index("dp")
    return me // (NC * NZ * NY), lax.rem(me // (NC * NZ), NY), lax.rem(me // NC, NZ), lax.rem(me, NC)


def index(x, y, z, c):
    return ((x * NY + y) * NZ + z) * NC + c


def after(z):
    return lax.rem(2 * z + 1, 5)


def before(z):
    return lax.rem(3 * z + 2, 5)


def partners():
    x, y, z, c = place()
    return {"x": index(1 - x, y, z, c), "y": index(x, 1 - y, z, c), "z": index(x, y, after(z), c), "c": index(x, y, z, 1 - c)}


def greet():
    x, y, z, c = place()
    barrier = pltpu.get_barrier_semaphore()
    others = [*partners().values(), index(x, y, before(z), c)]
    for other in others:
        pl.semaphore_signal(barrier, inc=1, device_id={"dp": other}, device_id_type=MESH)
    pl.semaphore_wait(barrier, len(others))


def rings():
    ring = [place()[2]]
    while len(ring) < NZ:
        ring.append(before(ring[-1]))
    return ring


class Copies:
    def __init__(self, send, recv, to):
        self.send, self.recv, self.to, self.made, self.number = send, recv, to, {}, {}

    def copy(self, src, dst, lane, name, way):
        number = self.number.setdefault(name, len(self.number))
        return pltpu.make_async_remote_copy(src_ref=src, dst_ref=dst, send_sem=self.send.at[lane], recv_sem=self.recv.at[number], device_id={"dp": self.to[way]}, device_id_type=MESH)

    def start(self, name, pair, way, lane, together=None):
        self.made[name] = (pair, way, lane)
        src, dst = pair()
        self.copy(src, dst, lane, together or name, way).start()

    def wait(self, name):
        pair, way, lane = self.made[name]
        src, dst = pair()
        self.copy(src, dst, lane, name, way).wait_recv()

    def wait_together(self, name, whole, way, lane):
        self.copy(whole, whole, lane, name, way).wait_recv()

    def finish(self, whole, way, lane):
        self.copy(whole, whole, lane, next(iter(self.number)), way).wait_send()


def gather_steps(copies, source, target, units, first, number):
    x, y, z, c = place()
    X, Y = 1 - x, 1 - y
    ring = rings()
    wire, die = range(2)

    def at():
        return pl.ds(first, number)

    def rows(colour):
        return pl.ds(*units[colour])

    def region(colour, xs, ys, k):
        return target.at[at(), xs, ys, ring[k], c, rows(colour)]

    def send(name, way, colour, xs, ys, k, mine=NO):
        copies.start(colour + name, lambda: (source.at[at(), rows(colour)] if mine else region(colour, xs, ys, k), region(colour, xs, ys, k)), way, wire)

    def share(colour, xs, ys, k):
        copies.start(f"s{len(copies.made)}", lambda: (region(colour, xs, ys, k), region(colour, xs, ys, k)), "c", die, "die")

    yield
    send("x", "x", "C", x, y, 0, YES)
    send("y", "y", "B", x, y, 0, YES)
    send("z1", "z", "A", x, y, 0, YES)
    send("x0", "x", "A", x, y, 0, YES)
    send("y0", "y", "A", x, y, 0, YES)
    copies.start("own", lambda: (source.at[at()], target.at[at(), x, y, z, c]), "c", die, "die")
    yield
    copies.wait("Cx")
    send("z1", "z", "C", ALL, y, 0)
    send("y0", "y", "C", ALL, y, 0)
    share("C", X, y, 0)
    yield
    copies.wait("By")
    send("z1", "z", "B", x, ALL, 0)
    send("x0", "x", "B", x, ALL, 0)
    share("B", x, Y, 0)
    for k in range(1, NZ):
        on = k < NZ - 1
        yield
        copies.wait(f"Az{k}")
        if on:
            send(f"z{k + 1}", "z", "A", x, y, k)
        send(f"x{k}", "x", "A", x, y, k)
        send(f"y{k}", "y", "A", x, y, k)
        share("A", x, y, k)
        yield
        copies.wait(f"Ax{k - 1}")
        send(f"Y{k - 1}", "y", "A", X, y, k - 1)
        share("A", X, y, k - 1)
        yield
        copies.wait(f"Cz{k}")
        if on:
            send(f"z{k + 1}", "z", "C", ALL, y, k)
        send(f"y{k}", "y", "C", ALL, y, k)
        share("C", ALL, y, k)
        yield
        copies.wait(f"Bz{k}")
        if on:
            send(f"z{k + 1}", "z", "B", x, ALL, k)
        send(f"x{k}", "x", "B", x, ALL, k)
        share("B", x, ALL, k)
    yield
    copies.wait(f"Ax{k}")
    send(f"Y{k}", "y", "A", X, y, k)
    share("A", X, y, k)
    for k in range(NZ):
        yield
        copies.wait(f"Bx{k}")
        share("B", X, ALL, k)
        yield
        copies.wait(f"Cy{k}")
        share("C", ALL, Y, k)
        yield
        copies.wait(f"Ay{k}")
        copies.wait(f"AY{k}")
        share("A", ALL, Y, k)
    yield
    flat = target.reshape(target.shape[0], CHIPS * NC, *target.shape[-3:])
    copies.wait_together("die", flat.at[at(), pl.ds(0, CHIPS)], "c", die)
    copies.finish(flat.at[at(), pl.ds(0, CHIPS)], "c", die)
    copies.finish(flat.at[at(), pl.ds(0, ARRIVALS)], "x", wire)


def add_pairs(dst, src, count, pairs):
    def body(m, _):
        for i, j in pairs:
            dst[(m, *i)] = (dst[(m, *i)].astype(F32) + src[(m, *j)].astype(F32)).astype(BF16)
        return 0
    lax.fori_loop(0, count, body, 0)


def scatter_steps(copies, count, terms, which, total, other, arrive, units):
    x, y, z, c = place()
    X, Y = 1 - x, 1 - y
    ring = rings()
    away = 1 - c
    slots, used = {}, dict.fromkeys("ABC", 0)
    lanes = {"A": 0, "B": 1, "C": 2, "die": 3}

    def half(colour, far):
        if colour == "B":
            return (X if far else x), ALL
        return ALL, (Y if far else y)

    def blocks(xs, ys):
        return [(e, ys) for e in range(NX)] if xs is ALL else [(xs, e) for e in range(NY)] if ys is ALL else [(xs, ys)]

    def swap(k, far):
        for colour in ("AC", "B"):
            def pair(colour=colour):
                xs, ys = half(colour, far)
                rows = pl.ds(*units[colour])
                return terms().at[which, xs, ys, ring[k], away, rows], other.at[ALL, xs, ys, ring[k], rows]
            copies.start(f"s{colour}{k}{far}", pair, "c", lanes["die"])

    def swapped(k, far):
        for colour in ("AC", "B"):
            copies.wait(f"s{colour}{k}{far}")
            a, n = units[colour]
            at = [(bx, by, ring[k], a + u) for bx, by in blocks(*half(colour, far)) for u in range(n)]
            add_pairs(total, other, count, [(i, i) for i in at])

    def send(name, way, colour, xs, ys, k):
        number, at = len(blocks(xs, ys)), used[colour]
        used[colour] += number
        slots[colour + name] = at

        def pair():
            return total.at[ALL, xs, ys, ring[k], pl.ds(*units[colour])], arrive[colour].at[ALL, pl.ds(at, number) if number > 1 else at]
        copies.start(colour + name, pair, way, lanes[colour])

    def take(name, colour, xs, ys, k):
        copies.wait(colour + name)
        (a, n), at = units[colour], slots[colour + name]
        add_pairs(total, arrive[colour], count, [((bx, by, ring[k], a + u), (at + e, u)) for e, (bx, by) in enumerate(blocks(xs, ys)) for u in range(n)])

    def far(k):
        swapped(k, YES)
        send(f"y{k}", "y", "A", ALL, Y, k)
        send(f"y{k}", "y", "C", ALL, Y, k)
        send(f"x{k}", "x", "B", X, ALL, k)

    def chain(colour, xs, ys, k):
        t = k or NZ
        if t > 1:
            take(f"z{t - 1}", colour, xs, ys, k)
        if t < NZ:
            send(f"z{t}", "z", colour, xs, ys, k)

    def second(k):
        take(f"y{k}", "A", ALL, y, k)
        send(f"x{k}", "x", "A", X, y, k)
        yield
        take(f"y{k}", "C", ALL, y, k)
        chain("C", ALL, y, k)
        if k == 0:
            send("x", "x", "C", X, y, k)
        yield
        take(f"x{k}", "B", x, ALL, k)
        chain("B", x, ALL, k)
        if k == 0:
            send("y", "y", "B", x, Y, k)

    def third(k):
        take(f"x{k}", "A", x, y, k)
        chain("A", x, y, k)

    order = [*range(1, NZ), 0]
    yield
    for k, distant in ((1, YES), (2, YES), (1, NO), (3, YES), (2, NO), (0, YES), (3, NO), (0, NO)):
        swap(k, distant)
    yield
    far(order[0])
    yield
    far(order[1])
    for at, k in enumerate(order):
        yield
        swapped(k, NO)
        if at:
            yield
            third(order[at - 1])
        yield
        yield from second(k)
        if at + 2 < NZ:
            yield
            far(order[at + 2])
    yield
    third(0)
    yield
    take("x", "C", x, y, 0)
    yield
    take("y", "B", x, y, 0)
    copies.finish(other, "c", lanes["die"])
    for colour in "ABC":
        copies.finish(arrive[colour], "x", lanes[colour])


class Clock:
    def __init__(self, runs):
        self.runs, self.on, self.done = runs, {}, {}
        for run in runs:
            next(run)

    def launch(self, i, begin, length):
        self.on[i] = (begin, length)
        self.done[i] = 0

    def due(self):
        return [(begin + length * self.done[i] / 29, i) for i, (begin, length) in self.on.items()]

    def step(self, i):
        self.done[i] += 1
        if next(self.runs[i], "end") == "end":
            del self.on[i]

    def advance(self, until):
        while self.on and min(self.due())[0] <= until:
            self.step(min(self.due())[1])

    def finish(self, i):
        while i in self.on:
            self.step(min(self.due())[1])


def nn(a, b):
    return jnp.dot(a, b, preferred_element_type=F32)


def nt(a, b):
    return lax.dot_general(a, b, (((1,), (1,)), ((), ())), preferred_element_type=F32)


def span(i, n):
    return pl.ds(pl.multiple_of(i * n, n), n)


def scale_of(wide):
    return lax.rsqrt(jnp.mean(wide * wide, -1, keepdims=True) + EPS)


def start(copy):
    copy.start()


def wait(copy):
    copy.wait()


def repeat(number, body):
    def one(i, _):
        body(i)
        return 0
    lax.fori_loop(0, number, one, 0)


FORWARD_TIMES = ((0, 26), (12, 20), (22, 30), (44, 20))
TILE_CLOCKS = ((27, 2.5), (58, 2.5))
DOWN_CLOCK = (45, 2)
WIDE = 512


def forward_kernel(x, gu_in, dn_in, gu, dn, h1, silu, slope, pt, h, a, p, wgu_t, wd, silu_t, slope_t, pt_t, gu_own, dn_own, send, recv, sem_in, sem_out, sem_h, local):
    greet()
    mx, my, mz, mc = place()
    to = partners()
    clock = Clock([gather_steps(Copies(send.at[2 * l + i], recv.at[2 * l + i], to), *which, (2 - i) * l, 2 - i)
                   for l in range(LAYERS) for i, which in enumerate(((gu_in, gu, GU_UNITS), (dn_in, dn, DN_UNITS)))])
    for i, times in enumerate(FORWARD_TIMES):
        clock.launch(i, *times)

    def mine(act, back):
        ways = [(gu_own, gu.at[ALL, mx, my, mz, mc]), (dn_own, dn.at[ALL, mx, my, mz, mc])] if back else [(gu_in, gu_own), (dn_in, dn_own)]
        for i, (src, dst) in enumerate(ways):
            act(pltpu.make_async_copy(src, dst, local.at[2 * back + i]))

    mine(start, 0)
    states = pltpu.make_async_copy(x, h, sem_h.at[0])
    states.start()
    clock.advance(0)
    mine(wait, 0)
    mine(start, 1)
    states.wait()
    mine(wait, 1)

    @pl.loop(0, TOKENS // TILE)
    def norm(t):
        wide = h[span(t, TILE), :].astype(F32)
        a[span(t, TILE), :] = (wide * scale_of(wide)).astype(BF16)

    clock.finish(0)

    def inputs(l, f, slot, act):
        for i in range(2):
            act(pltpu.make_async_copy(gu.at[2 * l + i].reshape(D, FF).at[:, span(f, TILE)], wgu_t.at[slot, :, pl.ds(i * TILE, TILE)], sem_in.at[slot, i]))

    def outputs(l, f, slot, act):
        act(pltpu.make_async_copy(silu_t.at[slot], silu.at[l, f], sem_out.at[slot, 0]))
        act(pltpu.make_async_copy(slope_t.at[slot], slope.at[l, f], sem_out.at[slot, 1]))
        act(pltpu.make_async_copy(pt_t.at[slot], pt.at[l, span(f, TILE), :], sem_out.at[slot, 2]))

    def hidden(l):
        inputs(l, 0, 0, start)

        def tile(f):
            slot = lax.rem(f, 2)
            inputs(l, f, slot, wait)

            @pl.when(f + 1 < TILES)
            def _():
                inputs(l, f + 1, 1 - slot, start)

            @pl.when(f > 1)
            def _():
                outputs(l, f - 2, slot, wait)

            for t in range(TOKENS // TILE):
                rows = pl.ds(t * TILE, TILE)
                both = nn(a[rows, :], wgu_t[slot])
                g, u = both[:, :TILE], both[:, TILE:]
                sig = 0.5 * jnp.tanh(0.5 * g) + 0.5
                s = g * sig
                out = s * u
                silu_t[slot, rows, :] = s
                slope_t[slot, rows, :] = u * (sig + s * (1.0 - sig))
                pt_t[slot, :, rows] = out.T.astype(BF16)
                if l == 0:
                    p[rows, span(f, TILE)] = out.astype(BF16)
            outputs(l, f, slot, start)
            for i in range(TILES):
                @pl.when(f == i)
                def _():
                    clock.advance(TILE_CLOCKS[l][0] + (i + 1) * TILE_CLOCKS[l][1])
        repeat(TILES, tile)
        for f in (TILES - 2, TILES - 1):
            outputs(l, f, f % 2, wait)

    hidden(0)
    clock.finish(1)
    down = pltpu.make_async_copy(dn.at[0].reshape(FF, D), wd, sem_h.at[1])
    down.start()
    down.wait()

    def second(t):
        rows = span(t, WIDE)
        new = (h[rows, :].astype(F32) + nn(p[rows, :], wd[ALL, ALL]).astype(BF16).astype(F32)).astype(BF16)
        h[rows, :] = new
        wide = new.astype(F32)
        a[rows, :] = (wide * scale_of(wide)).astype(BF16)
        for i in range(TOKENS // WIDE):
            @pl.when(t == i)
            def _():
                clock.advance(DOWN_CLOCK[0] + (i + 1) * DOWN_CLOCK[1])
    repeat(TOKENS // WIDE, second)
    states = pltpu.make_async_copy(h, h1, sem_h.at[0])
    states.start()
    clock.finish(2)
    hidden(1)
    clock.finish(3)
    states.wait()


GATHER_RECV = 32


def forward(x, gu_in, dn_in):
    hbm = pl.BlockSpec(memory_space=pl.ANY)
    vmem, dma = pltpu.VMEM, pltpu.SemaphoreType.DMA
    wide = jax.ShapeDtypeStruct((LAYERS, TILES, TOKENS, TILE), F32)
    double = vmem((2, TOKENS, TILE), F32)
    return pl.pallas_call(
        forward_kernel, name="forward",
        out_shape=(jax.ShapeDtypeStruct((2 * LAYERS, *GRID, *gu_in.shape[1:]), BF16), jax.ShapeDtypeStruct((LAYERS, *GRID, *dn_in.shape[1:]), BF16),
                   jax.ShapeDtypeStruct((TOKENS, D), BF16), wide, wide, jax.ShapeDtypeStruct((LAYERS, FF, TOKENS), BF16)),
        in_specs=[hbm] * 3, out_specs=(hbm,) * 6,
        scratch_shapes=[vmem((TOKENS, D), BF16), vmem((TOKENS, D), BF16), vmem((TOKENS, FF), BF16), vmem((2, D, 2 * TILE), BF16), vmem((FF, D), BF16),
                        double, double, vmem((2, TILE, TOKENS), BF16), vmem(gu_in.shape, BF16), vmem(dn_in.shape, BF16),
                        dma((2 * LAYERS, 2)), dma((2 * LAYERS, GATHER_RECV)), dma((2, 2)), dma((2, 3)), dma((2,)), dma((4,))],
        compiler_params=pltpu.CompilerParams(collective_id=0, has_side_effects=YES, vmem_limit_bytes=LIMIT),
    )(x, gu_in, dn_in)


BACK_TIMES = ((45, 26), (58, 16), (67, 24), (76, 16))
GRADS_CLOCK = (46, 3)
LATE_DOWN_CLOCK = (67, 1)
LATE_STATES_CLOCK = (74, 2)


def back_kernel(dy, h0, h1, wgu, wd, silu, slope, pt, dx, gu_out, dn_out, gus, dns, late,
                ct, hbuf, at, acc, gate, up, wgu_t, wd_t, p, dgu, stage, stage_dn,
                gu1, gx1, ga1, gb1, gc1, dn1, dx1, da1, db1, dc1, gu0, gx0, ga0, gb0, gc0, dn0, dx0, da0, db0, dc0,
                send, recv, sem_in, sem_h, sem_out, sem_late, sem_own):
    greet()
    to = partners()
    mx, my, mz, mc = place()
    collect = []
    for l, sets in ((1, ((gu1, gx1, ga1, gb1, gc1), (dn1, dx1, da1, db1, dc1))), (0, ((gu0, gx0, ga0, gb0, gc0), (dn0, dx0, da0, db0, dc0)))):
        for i, (total, other, *slots) in enumerate(sets):
            def terms(l=l, i=i):
                return dns.reshape(LAYERS, *GRID, DN_UNITS["all"], ROWS, D) if i else gus.reshape(2 * LAYERS, *GRID, GU_UNITS["all"], ROWS, FF)

            which = pl.ds(l, 1) if i else pl.ds(2 * l, 2)

            def own(total=total, terms=terms, which=which, number=len(collect)):
                return pltpu.make_async_copy(terms().at[which, ALL, ALL, ALL, mc], total, sem_own.at[number])

            def away(total=total, l=l, i=i, number=len(collect)):
                here = total.at[ALL, mx, my, mz]
                return pltpu.make_async_copy(here, dn_out.at[pl.ds(l, 1)] if i else gu_out.at[pl.ds(2 * l, 2)], sem_own.at[number])
            n = len(collect)
            steps = scatter_steps(Copies(send.at[n], recv.at[n], to), 2 - i, terms, which, total, other, dict(zip("ABC", slots)), DN_UNITS if i else GU_UNITS)
            collect.append((steps, own, away))
    clock = Clock([one[0] for one in collect])

    def launch(i):
        collect[i][1]().start()
        clock.launch(i, *BACK_TIMES[i])
        clock.step(i)

    def ready(i):
        collect[i][1]().wait()

    def inputs(step, slot, act):
        l, f = 1 - step // TILES, lax.rem(step, TILES)
        cols = span(f, TILE)
        copies = [(wgu.at[2 * l, :, cols], wgu_t.at[slot, :, pl.ds(0, TILE)]), (wgu.at[2 * l + 1, :, cols], wgu_t.at[slot, :, pl.ds(TILE, TILE)]),
                  (wd.at[l, cols, :], wd_t.at[slot]), (silu.at[l, f], gate.at[slot]), (slope.at[l, f], up.at[slot]), (pt.at[l, cols, :], p.at[slot])]
        for i, (src, dst) in enumerate(copies):
            act(pltpu.make_async_copy(src, dst, sem_in.at[slot, i]))

    def outputs(l, f, act):
        act(pltpu.make_async_copy(stage.at[:, pl.ds(0, TILE)], gus.at[2 * l, :, span(f, TILE)], sem_out.at[0]))
        act(pltpu.make_async_copy(stage.at[:, pl.ds(TILE, TILE)], gus.at[2 * l + 1, :, span(f, TILE)], sem_out.at[1]))

    def down_output(l, f, act):
        act(pltpu.make_async_copy(stage_dn, dns.at[l, span(f, TILE), :], sem_out.at[2]))

    def late_copy(f, slot, act, back):
        ends = (late.at[f], dgu.at[slot]) if back else (dgu.at[slot], late.at[f])
        act(pltpu.make_async_copy(*ends, sem_late.at[slot]))

    def states_back(slot):
        half = TOKENS // 2

        @pl.loop(0, 2)
        def _(t):
            acc[span(t, half), :] += nt(dgu[slot, span(t, half), :], wgu_t[slot])

    def norm_back():
        @pl.loop(0, TOKENS // TILE)
        def _(t):
            rows = span(t, TILE)
            wide = hbuf[rows, :].astype(F32)
            s = scale_of(wide)
            n, by_a = wide * s, acc[rows, :]
            by_h = s * (by_a - n * jnp.mean(by_a * n, -1, keepdims=True))
            ct[rows, :] = (ct[rows, :].astype(F32) + by_h).astype(BF16)

    first = pltpu.make_async_copy(dy, ct, sem_h.at[0])
    first.start()
    pltpu.make_async_copy(h1, hbuf, sem_h.at[1]).start()
    inputs(0, 0, start)
    first.wait()

    def body(step):
        l, f, slot = 1 - step // TILES, lax.rem(step, TILES), lax.rem(step, 2)
        inputs(step, slot, wait)

        @pl.when(step + 1 < 2 * TILES)
        def _():
            inputs(step + 1, 1 - slot, start)

        @pl.when(f == 0)
        def _():
            pltpu.make_async_copy(h1, hbuf, sem_h.at[1]).wait()

            @pl.loop(0, TOKENS // TILE)
            def _(t):
                rows = span(t, TILE)
                wide = hbuf[rows, :].astype(F32)
                at[:, rows] = (wide * scale_of(wide)).T.astype(BF16)
                acc[rows, :] = jnp.zeros((TILE, D), F32)

        @pl.when(step > TILES + 1)
        def _():
            late_copy(f - 2, slot, wait, NO)

        @pl.loop(0, 2)
        def _(t):
            rows = span(t, TOKENS // 2)
            by_p = nt(ct[rows, :], wd_t[slot]).astype(BF16).astype(F32)
            dgu[slot, rows, pl.ds(0, TILE)] = (by_p * up[slot, rows, :]).astype(BF16)
            dgu[slot, rows, pl.ds(TILE, TILE)] = (by_p * gate[slot, rows, :]).astype(BF16)

        @pl.when(f > 0)
        def _():
            outputs(l, f - 1, wait)
        stage[ALL, ALL] = nn(at[ALL, ALL], dgu[slot]).astype(BF16)
        outputs(l, f, start)

        @pl.when(l == 0)
        def _():
            late_copy(f, slot, start, NO)

        @pl.when(l == 1)
        def _():
            @pl.when(f > 0)
            def _():
                down_output(l, f - 1, wait)
            stage_dn[ALL, ALL] = nn(p[slot], ct[ALL, ALL]).astype(BF16)
            down_output(l, f, start)
            states_back(slot)

        @pl.when(step == TILES - 1)
        def _():
            outputs(l, f, wait)
            launch(0)
            down_output(l, f, wait)
            launch(1)
            norm_back()
            pltpu.make_async_copy(h0, hbuf, sem_h.at[1]).start()
            ready(0)
            ready(1)

        for i in range(TILES):
            @pl.when(step == TILES + i)
            def _():
                clock.advance(GRADS_CLOCK[0] + (i + 1) * GRADS_CLOCK[1])

    repeat(2 * TILES, body)
    outputs(0, TILES - 1, wait)
    launch(2)
    for f in (TILES - 2, TILES - 1):
        late_copy(f, (f + TILES) % 2, wait, NO)

    def again(f, slot, act, which):
        if which:
            late_copy(f, slot, act, YES)
            for i in range(2):
                act(pltpu.make_async_copy(wgu.at[i, :, span(f, TILE)], wgu_t.at[slot, :, pl.ds(i * TILE, TILE)], sem_in.at[slot, i]))
        else:
            act(pltpu.make_async_copy(pt.at[0, span(f, TILE), :], p.at[slot], sem_in.at[slot, 2]))

    again(0, 0, start, NO)
    again(0, 0, start, YES)
    ready(2)

    def late_down(f):
        slot = lax.rem(f, 2)
        again(f, slot, wait, NO)

        @pl.when(f + 1 < TILES)
        def _():
            again(f + 1, 1 - slot, start, NO)

        @pl.when(f > 0)
        def _():
            down_output(0, f - 1, wait)
        stage_dn[ALL, ALL] = nn(p[slot], ct[ALL, ALL]).astype(BF16)
        down_output(0, f, start)
        for i in range(TILES):
            @pl.when(f == i)
            def _():
                clock.advance(LATE_DOWN_CLOCK[0] + (i + 1) * LATE_DOWN_CLOCK[1])
    repeat(TILES, late_down)
    down_output(0, TILES - 1, wait)
    launch(3)

    def late_states(f):
        slot = lax.rem(f, 2)
        again(f, slot, wait, YES)

        @pl.when(f + 1 < TILES)
        def _():
            again(f + 1, 1 - slot, start, YES)
        states_back(slot)

        @pl.when(f == 0)
        def _():
            ready(3)
        for i in range(TILES):
            @pl.when(f == i)
            def _():
                clock.advance(LATE_STATES_CLOCK[0] + (i + 1) * LATE_STATES_CLOCK[1])
    repeat(TILES, late_states)
    norm_back()
    last = pltpu.make_async_copy(ct, dx, sem_h.at[0])
    last.start()
    for i in range(len(collect)):
        clock.finish(i)
    for act in (start, wait):
        for one in collect:
            act(one[-1]())
    last.wait()


SCATTER_RECV = 43


def back(dy, h0, h1, wgu, wd, silu, slope, pt):
    hbm = pl.BlockSpec(memory_space=pl.ANY)
    vmem, dma = pltpu.VMEM, pltpu.SemaphoreType.DMA
    buffers = []
    for count, units, columns in ((2, GU_UNITS, FF), (1, DN_UNITS, D)):
        whole = vmem((count, NX, NY, NZ, units["all"], ROWS, columns), BF16)
        buffers += [whole, whole, *(vmem((count, ARRIVALS, units[colour][1], ROWS, columns), BF16) for colour in "ABC")]
    double, states = vmem((2, TOKENS, TILE), F32), vmem((TOKENS, D), BF16)
    return pl.pallas_call(
        back_kernel, name="back",
        out_shape=(jax.ShapeDtypeStruct((TOKENS, D), BF16), jax.ShapeDtypeStruct((2 * LAYERS, GU_UNITS["all"], ROWS, FF), BF16),
                   jax.ShapeDtypeStruct((LAYERS, DN_UNITS["all"], ROWS, D), BF16), jax.ShapeDtypeStruct((2 * LAYERS, D, FF), BF16),
                   jax.ShapeDtypeStruct((LAYERS, FF, D), BF16), jax.ShapeDtypeStruct((TILES, TOKENS, 2 * TILE), BF16)),
        in_specs=[hbm] * 8, out_specs=(hbm,) * 6,
        scratch_shapes=[states, states, vmem((D, TOKENS), BF16), vmem((TOKENS, D), F32), double, double, vmem((2, D, 2 * TILE), BF16), vmem((2, TILE, D), BF16),
                        vmem((2, TILE, TOKENS), BF16), vmem((2, TOKENS, 2 * TILE), BF16), vmem((D, 2 * TILE), BF16), vmem((TILE, D), BF16), *buffers, *buffers,
                        dma((4, 4)), dma((4, SCATTER_RECV)), dma((2, 6)), dma((2,)), dma((3,)), dma((2,)), dma((4,))],
        compiler_params=pltpu.CompilerParams(collective_id=1, has_side_effects=YES, vmem_limit_bytes=LIMIT),
    )(dy, h0, h1, wgu, wd, silu, slope, pt)[:3]


def solution(mesh):
    def step(x, dy, w_gate, w_up, w_down):
        gu_in = jnp.stack([w_gate, w_up], 1).reshape(2 * LAYERS, GU_UNITS["all"], ROWS, FF)
        x, dy = x[0], dy[0]
        gu, dn, h, silu, slope, pt = forward(x, gu_in, w_down.reshape(LAYERS, DN_UNITS["all"], ROWS, D))
        dx, by_gu, by_dn = back(dy, x, h, gu.reshape(2 * LAYERS, D, FF), dn.reshape(LAYERS, FF, D), silu, slope, pt)
        by_gu = by_gu.reshape(w_gate.shape[0], 2, *w_gate.shape[1:])
        return dx[None], by_gu[:, 0], by_gu[:, 1], by_dn.reshape(w_down.shape)

    rows = P(None, "dp", None)
    tokens, grads = P(("rep", "dp"), None, None), P("rep", "dp", None)
    return jax.shard_map(step, mesh=mesh, in_specs=(tokens, tokens, rows, rows, rows), out_specs=(tokens, grads, grads, grads), check_vma=NO)
```

```python
import jax
import jax.numpy as jnp
from jax import lax
from jax.experimental import pallas as pl
from jax.experimental.pallas import tpu as pltpu
from jax.sharding import PartitionSpec as P

F32 = jnp.float32
BF16 = jnp.bfloat16
LAYERS, TOKENS, D, FF = 2, 2048, 768, 1792
NX, NY, NZ, NC = GRID = (2, 2, 4, 2)
ROWS = 8
GU_UNITS = {"A": (0, 1), "C": (1, 1), "B": (2, 1), "AC": (0, 2), "all": 3}
DN_UNITS = {"A": (0, 2), "C": (2, 2), "B": (4, 3), "AC": (0, 4), "all": 7}
ALL = slice(None)
YES, NO = True, False
MESH = pl.DeviceIdType.MESH
CHIPS = NX * NY * NZ
ARRIVALS = CHIPS - 1
TILE = 256
TILES = FF // TILE
EPS = 1e-6
LIMIT = 63 * 2**20


def place():
    me = lax.axis_index("dp")
    return me // (NC * NZ * NY), lax.rem(me // (NC * NZ), NY), lax.rem(me // NC, NZ), lax.rem(me, NC)


def index(x, y, z, c):
    return ((x * NY + y) * NZ + z) * NC + c


def after(z):
    return lax.rem(2 * z + 1, 5)


def before(z):
    return lax.rem(3 * z + 2, 5)


def partners():
    x, y, z, c = place()
    return {"x": index(1 - x, y, z, c), "y": index(x, 1 - y, z, c), "z": index(x, y, after(z), c), "c": index(x, y, z, 1 - c)}


def greet():
    x, y, z, c = place()
    barrier = pltpu.get_barrier_semaphore()
    others = [*partners().values(), index(x, y, before(z), c)]
    for other in others:
        pl.semaphore_signal(barrier, inc=1, device_id={"dp": other}, device_id_type=MESH)
    pl.semaphore_wait(barrier, len(others))


def rings():
    ring = [place()[2]]
    while len(ring) < NZ:
        ring.append(before(ring[-1]))
    return ring


class Copies:
    def __init__(self, send, recv, to):
        self.send, self.recv, self.to, self.made, self.number = send, recv, to, {}, {}

    def copy(self, src, dst, lane, name, way):
        number = self.number.setdefault(name, len(self.number))
        return pltpu.make_async_remote_copy(src_ref=src, dst_ref=dst, send_sem=self.send.at[lane], recv_sem=self.recv.at[number], device_id={"dp": self.to[way]}, device_id_type=MESH)

    def start(self, name, pair, way, lane, together=None):
        self.made[name] = (pair, way, lane)
        src, dst = pair()
        self.copy(src, dst, lane, together or name, way).start()

    def wait(self, name):
        pair, way, lane = self.made[name]
        src, dst = pair()
        self.copy(src, dst, lane, name, way).wait_recv()

    def wait_together(self, name, whole, way, lane):
        self.copy(whole, whole, lane, name, way).wait_recv()

    def finish(self, whole, way, lane):
        self.copy(whole, whole, lane, next(iter(self.number)), way).wait_send()


def gather_steps(copies, source, target, units, first, number):
    x, y, z, c = place()
    X, Y = 1 - x, 1 - y
    ring = rings()
    wire, die = range(2)

    def at():
        return pl.ds(first, number)

    def rows(colour):
        return pl.ds(*units[colour])

    def region(colour, xs, ys, k):
        return target.at[at(), xs, ys, ring[k], c, rows(colour)]

    def send(name, way, colour, xs, ys, k, mine=NO):
        copies.start(colour + name, lambda: (source.at[at(), rows(colour)] if mine else region(colour, xs, ys, k), region(colour, xs, ys, k)), way, wire)

    def share(colour, xs, ys, k):
        copies.start(f"s{len(copies.made)}", lambda: (region(colour, xs, ys, k), region(colour, xs, ys, k)), "c", die, "die")

    yield
    send("x", "x", "C", x, y, 0, YES)
    send("y", "y", "B", x, y, 0, YES)
    send("z1", "z", "A", x, y, 0, YES)
    send("x0", "x", "A", x, y, 0, YES)
    send("y0", "y", "A", x, y, 0, YES)
    copies.start("own", lambda: (source.at[at()], target.at[at(), x, y, z, c]), "c", die, "die")
    yield
    copies.wait("Cx")
    send("z1", "z", "C", ALL, y, 0)
    send("y0", "y", "C", ALL, y, 0)
    share("C", X, y, 0)
    yield
    copies.wait("By")
    send("z1", "z", "B", x, ALL, 0)
    send("x0", "x", "B", x, ALL, 0)
    share("B", x, Y, 0)
    for k in range(1, NZ):
        on = k < NZ - 1
        yield
        copies.wait(f"Az{k}")
        if on:
            send(f"z{k + 1}", "z", "A", x, y, k)
        send(f"x{k}", "x", "A", x, y, k)
        send(f"y{k}", "y", "A", x, y, k)
        share("A", x, y, k)
        yield
        copies.wait(f"Ax{k - 1}")
        send(f"Y{k - 1}", "y", "A", X, y, k - 1)
        share("A", X, y, k - 1)
        yield
        copies.wait(f"Cz{k}")
        if on:
            send(f"z{k + 1}", "z", "C", ALL, y, k)
        send(f"y{k}", "y", "C", ALL, y, k)
        share("C", ALL, y, k)
        yield
        copies.wait(f"Bz{k}")
        if on:
            send(f"z{k + 1}", "z", "B", x, ALL, k)
        send(f"x{k}", "x", "B", x, ALL, k)
        share("B", x, ALL, k)
    yield
    copies.wait(f"Ax{k}")
    send(f"Y{k}", "y", "A", X, y, k)
    share("A", X, y, k)
    for k in range(NZ):
        yield
        copies.wait(f"Bx{k}")
        share("B", X, ALL, k)
        yield
        copies.wait(f"Cy{k}")
        share("C", ALL, Y, k)
        yield
        copies.wait(f"Ay{k}")
        copies.wait(f"AY{k}")
        share("A", ALL, Y, k)
    yield
    flat = target.reshape(target.shape[0], CHIPS * NC, *target.shape[-3:])
    copies.wait_together("die", flat.at[at(), pl.ds(0, CHIPS)], "c", die)
    copies.finish(flat.at[at(), pl.ds(0, CHIPS)], "c", die)
    copies.finish(flat.at[at(), pl.ds(0, ARRIVALS)], "x", wire)


def add_pairs(dst, src, count, pairs):
    def body(m, _):
        for i, j in pairs:
            dst[(m, *i)] = (dst[(m, *i)].astype(F32) + src[(m, *j)].astype(F32)).astype(BF16)
        return 0
    lax.fori_loop(0, count, body, 0)


def scatter_steps(copies, count, terms, which, total, other, arrive, units):
    x, y, z, c = place()
    X, Y = 1 - x, 1 - y
    ring = rings()
    away = 1 - c
    slots, used = {}, dict.fromkeys("ABC", 0)
    lanes = {"A": 0, "B": 1, "C": 2, "die": 3}

    def half(colour, far):
        if colour == "B":
            return (X if far else x), ALL
        return ALL, (Y if far else y)

    def blocks(xs, ys):
        return [(e, ys) for e in range(NX)] if xs is ALL else [(xs, e) for e in range(NY)] if ys is ALL else [(xs, ys)]

    def swap(k, far):
        for colour in ("AC", "B"):
            def pair(colour=colour):
                xs, ys = half(colour, far)
                rows = pl.ds(*units[colour])
                return terms().at[which, xs, ys, ring[k], away, rows], other.at[ALL, xs, ys, ring[k], rows]
            copies.start(f"s{colour}{k}{far}", pair, "c", lanes["die"])

    def swapped(k, far):
        for colour in ("AC", "B"):
            copies.wait(f"s{colour}{k}{far}")
            a, n = units[colour]
            at = [(bx, by, ring[k], a + u) for bx, by in blocks(*half(colour, far)) for u in range(n)]
            add_pairs(total, other, count, [(i, i) for i in at])

    def send(name, way, colour, xs, ys, k):
        number, at = len(blocks(xs, ys)), used[colour]
        used[colour] += number
        slots[colour + name] = at

        def pair():
            return total.at[ALL, xs, ys, ring[k], pl.ds(*units[colour])], arrive[colour].at[ALL, pl.ds(at, number) if number > 1 else at]
        copies.start(colour + name, pair, way, lanes[colour])

    def take(name, colour, xs, ys, k):
        copies.wait(colour + name)
        (a, n), at = units[colour], slots[colour + name]
        add_pairs(total, arrive[colour], count, [((bx, by, ring[k], a + u), (at + e, u)) for e, (bx, by) in enumerate(blocks(xs, ys)) for u in range(n)])

    def far(k):
        swapped(k, YES)
        send(f"y{k}", "y", "A", ALL, Y, k)
        send(f"y{k}", "y", "C", ALL, Y, k)
        send(f"x{k}", "x", "B", X, ALL, k)

    def chain(colour, xs, ys, k):
        t = k or NZ
        if t > 1:
            take(f"z{t - 1}", colour, xs, ys, k)
        if t < NZ:
            send(f"z{t}", "z", colour, xs, ys, k)

    def second(k):
        take(f"y{k}", "A", ALL, y, k)
        send(f"x{k}", "x", "A", X, y, k)
        yield
        take(f"y{k}", "C", ALL, y, k)
        chain("C", ALL, y, k)
        if k == 0:
            send("x", "x", "C", X, y, k)
        yield
        take(f"x{k}", "B", x, ALL, k)
        chain("B", x, ALL, k)
        if k == 0:
            send("y", "y", "B", x, Y, k)

    def third(k):
        take(f"x{k}", "A", x, y, k)
        chain("A", x, y, k)

    order = [*range(1, NZ), 0]
    yield
    for k, distant in ((1, YES), (2, YES), (1, NO), (3, YES), (2, NO), (0, YES), (3, NO), (0, NO)):
        swap(k, distant)
    yield
    far(order[0])
    yield
    far(order[1])
    for at, k in enumerate(order):
        yield
        swapped(k, NO)
        if at:
            yield
            third(order[at - 1])
        yield
        yield from second(k)
        if at + 2 < NZ:
            yield
            far(order[at + 2])
    yield
    third(0)
    yield
    take("x", "C", x, y, 0)
    yield
    take("y", "B", x, y, 0)
    copies.finish(other, "c", lanes["die"])
    for colour in "ABC":
        copies.finish(arrive[colour], "x", lanes[colour])


class Clock:
    def __init__(self, runs):
        self.runs, self.on, self.done = runs, {}, {}
        for run in runs:
            next(run)

    def launch(self, i, begin, length):
        self.on[i] = (begin, length)
        self.done[i] = 0

    def due(self):
        return [(begin + length * self.done[i] / 29, i) for i, (begin, length) in self.on.items()]

    def step(self, i):
        self.done[i] += 1
        if next(self.runs[i], "end") == "end":
            del self.on[i]

    def advance(self, until):
        while self.on and min(self.due())[0] <= until:
            self.step(min(self.due())[1])

    def finish(self, i):
        while i in self.on:
            self.step(min(self.due())[1])


def nn(a, b):
    return jnp.dot(a, b, preferred_element_type=F32)


def nt(a, b):
    return lax.dot_general(a, b, (((1,), (1,)), ((), ())), preferred_element_type=F32)


def span(i, n):
    return pl.ds(pl.multiple_of(i * n, n), n)


def scale_of(wide):
    return lax.rsqrt(jnp.mean(wide * wide, -1, keepdims=True) + EPS)


def start(copy):
    copy.start()


def wait(copy):
    copy.wait()


def repeat(number, body):
    def one(i, _):
        body(i)
        return 0
    lax.fori_loop(0, number, one, 0)


FORWARD_TIMES = ((0, 22), (6, 22), (14, 40), (20, 55))
TILE_CLOCKS = ((24, 4), (60, 4))
DOWN_CLOCK = (52, 3)
WIDE = 512


def forward_kernel(x, gu_in, dn_in, gu, dn, h1, silu, slope, pt, h, a, p, wgu_t, wd, silu_t, slope_t, pt_t, gu_own, dn_own, send, recv, sem_in, sem_out, sem_h, local):
    greet()
    mx, my, mz, mc = place()
    to = partners()
    clock = Clock([gather_steps(Copies(send.at[2 * l + i], recv.at[2 * l + i], to), *which, (2 - i) * l, 2 - i)
                   for l in range(LAYERS) for i, which in enumerate(((gu_in, gu, GU_UNITS), (dn_in, dn, DN_UNITS)))])
    for i, times in enumerate(FORWARD_TIMES):
        clock.launch(i, *times)

    def mine(act, back):
        ways = [(gu_own, gu.at[ALL, mx, my, mz, mc]), (dn_own, dn.at[ALL, mx, my, mz, mc])] if back else [(gu_in, gu_own), (dn_in, dn_own)]
        for i, (src, dst) in enumerate(ways):
            act(pltpu.make_async_copy(src, dst, local.at[2 * back + i]))

    mine(start, 0)
    states = pltpu.make_async_copy(x, h, sem_h.at[0])
    states.start()
    clock.advance(0)
    mine(wait, 0)
    mine(start, 1)
    states.wait()
    mine(wait, 1)

    @pl.loop(0, TOKENS // TILE)
    def norm(t):
        wide = h[span(t, TILE), :].astype(F32)
        a[span(t, TILE), :] = (wide * scale_of(wide)).astype(BF16)

    clock.finish(0)

    def inputs(l, f, slot, act):
        for i in range(2):
            act(pltpu.make_async_copy(gu.at[2 * l + i].reshape(D, FF).at[:, span(f, TILE)], wgu_t.at[slot, :, pl.ds(i * TILE, TILE)], sem_in.at[slot, i]))

    def outputs(l, f, slot, act):
        act(pltpu.make_async_copy(silu_t.at[slot], silu.at[l, f], sem_out.at[slot, 0]))
        act(pltpu.make_async_copy(slope_t.at[slot], slope.at[l, f], sem_out.at[slot, 1]))
        act(pltpu.make_async_copy(pt_t.at[slot], pt.at[l, span(f, TILE), :], sem_out.at[slot, 2]))

    def hidden(l):
        inputs(l, 0, 0, start)

        def tile(f):
            slot = lax.rem(f, 2)
            inputs(l, f, slot, wait)

            @pl.when(f + 1 < TILES)
            def _():
                inputs(l, f + 1, 1 - slot, start)

            @pl.when(f > 1)
            def _():
                outputs(l, f - 2, slot, wait)

            for t in range(TOKENS // TILE):
                rows = pl.ds(t * TILE, TILE)
                both = nn(a[rows, :], wgu_t[slot])
                g, u = both[:, :TILE], both[:, TILE:]
                sig = 0.5 * jnp.tanh(0.5 * g) + 0.5
                s = g * sig
                out = s * u
                silu_t[slot, rows, :] = s
                slope_t[slot, rows, :] = u * (sig + s * (1.0 - sig))
                pt_t[slot, :, rows] = out.T.astype(BF16)
                if l == 0:
                    p[rows, span(f, TILE)] = out.astype(BF16)
            outputs(l, f, slot, start)
            for i in range(TILES):
                @pl.when(f == i)
                def _():
                    clock.advance(TILE_CLOCKS[l][0] + (i + 1) * TILE_CLOCKS[l][1])
        repeat(TILES, tile)
        for f in (TILES - 2, TILES - 1):
            outputs(l, f, f % 2, wait)

    hidden(0)
    clock.finish(1)
    down = pltpu.make_async_copy(dn.at[0].reshape(FF, D), wd, sem_h.at[1])
    down.start()
    down.wait()

    def second(t):
        rows = span(t, WIDE)
        new = (h[rows, :].astype(F32) + nn(p[rows, :], wd[ALL, ALL]).astype(BF16).astype(F32)).astype(BF16)
        h[rows, :] = new
        wide = new.astype(F32)
        a[rows, :] = (wide * scale_of(wide)).astype(BF16)
        for i in range(TOKENS // WIDE):
            @pl.when(t == i)
            def _():
                clock.advance(DOWN_CLOCK[0] + (i + 1) * DOWN_CLOCK[1])
    repeat(TOKENS // WIDE, second)
    states = pltpu.make_async_copy(h, h1, sem_h.at[0])
    states.start()
    clock.finish(2)
    hidden(1)
    clock.finish(3)
    states.wait()


GATHER_RECV = 32


def forward(x, gu_in, dn_in):
    hbm = pl.BlockSpec(memory_space=pl.ANY)
    vmem, dma = pltpu.VMEM, pltpu.SemaphoreType.DMA
    wide = jax.ShapeDtypeStruct((LAYERS, TILES, TOKENS, TILE), F32)
    double = vmem((2, TOKENS, TILE), F32)
    return pl.pallas_call(
        forward_kernel, name="forward",
        out_shape=(jax.ShapeDtypeStruct((2 * LAYERS, *GRID, *gu_in.shape[1:]), BF16), jax.ShapeDtypeStruct((LAYERS, *GRID, *dn_in.shape[1:]), BF16),
                   jax.ShapeDtypeStruct((TOKENS, D), BF16), wide, wide, jax.ShapeDtypeStruct((LAYERS, FF, TOKENS), BF16)),
        in_specs=[hbm] * 3, out_specs=(hbm,) * 6,
        scratch_shapes=[vmem((TOKENS, D), BF16), vmem((TOKENS, D), BF16), vmem((TOKENS, FF), BF16), vmem((2, D, 2 * TILE), BF16), vmem((FF, D), BF16),
                        double, double, vmem((2, TILE, TOKENS), BF16), vmem(gu_in.shape, BF16), vmem(dn_in.shape, BF16),
                        dma((2 * LAYERS, 2)), dma((2 * LAYERS, GATHER_RECV)), dma((2, 2)), dma((2, 3)), dma((2,)), dma((4,))],
        compiler_params=pltpu.CompilerParams(collective_id=0, has_side_effects=YES, vmem_limit_bytes=LIMIT),
    )(x, gu_in, dn_in)


BACK_TIMES = ((45, 34), (50, 30), (67, 30), (76, 26))
GRADS_CLOCK = (46, 3)
LATE_DOWN_CLOCK = (67, 1)
LATE_STATES_CLOCK = (74, 2)


def back_kernel(dy, h0, h1, wgu, wd, silu, slope, pt, dx, gu_out, dn_out, gus, dns, late,
                ct, hbuf, at, acc, gate, up, wgu_t, wd_t, p, dgu, stage, stage_dn,
                gu1, gx1, ga1, gb1, gc1, dn1, dx1, da1, db1, dc1, gu0, gx0, ga0, gb0, gc0, dn0, dx0, da0, db0, dc0,
                send, recv, sem_in, sem_h, sem_out, sem_late, sem_own):
    greet()
    to = partners()
    mx, my, mz, mc = place()
    collect = []
    for l, sets in ((1, ((gu1, gx1, ga1, gb1, gc1), (dn1, dx1, da1, db1, dc1))), (0, ((gu0, gx0, ga0, gb0, gc0), (dn0, dx0, da0, db0, dc0)))):
        for i, (total, other, *slots) in enumerate(sets):
            def terms(l=l, i=i):
                return dns.reshape(LAYERS, *GRID, DN_UNITS["all"], ROWS, D) if i else gus.reshape(2 * LAYERS, *GRID, GU_UNITS["all"], ROWS, FF)

            which = pl.ds(l, 1) if i else pl.ds(2 * l, 2)

            def own(total=total, terms=terms, which=which, number=len(collect)):
                return pltpu.make_async_copy(terms().at[which, ALL, ALL, ALL, mc], total, sem_own.at[number])

            def away(total=total, l=l, i=i, number=len(collect)):
                here = total.at[ALL, mx, my, mz]
                return pltpu.make_async_copy(here, dn_out.at[pl.ds(l, 1)] if i else gu_out.at[pl.ds(2 * l, 2)], sem_own.at[number])
            n = len(collect)
            steps = scatter_steps(Copies(send.at[n], recv.at[n], to), 2 - i, terms, which, total, other, dict(zip("ABC", slots)), DN_UNITS if i else GU_UNITS)
            collect.append((steps, own, away))
    clock = Clock([one[0] for one in collect])

    def launch(i):
        collect[i][1]().start()
        clock.launch(i, *BACK_TIMES[i])
        clock.step(i)

    def ready(i):
        collect[i][1]().wait()

    def inputs(step, slot, act):
        l, f = 1 - step // TILES, lax.rem(step, TILES)
        cols = span(f, TILE)
        copies = [(wgu.at[2 * l, :, cols], wgu_t.at[slot, :, pl.ds(0, TILE)]), (wgu.at[2 * l + 1, :, cols], wgu_t.at[slot, :, pl.ds(TILE, TILE)]),
                  (wd.at[l, cols, :], wd_t.at[slot]), (silu.at[l, f], gate.at[slot]), (slope.at[l, f], up.at[slot]), (pt.at[l, cols, :], p.at[slot])]
        for i, (src, dst) in enumerate(copies):
            act(pltpu.make_async_copy(src, dst, sem_in.at[slot, i]))

    def outputs(l, f, act):
        act(pltpu.make_async_copy(stage.at[:, pl.ds(0, TILE)], gus.at[2 * l, :, span(f, TILE)], sem_out.at[0]))
        act(pltpu.make_async_copy(stage.at[:, pl.ds(TILE, TILE)], gus.at[2 * l + 1, :, span(f, TILE)], sem_out.at[1]))

    def down_output(l, f, act):
        act(pltpu.make_async_copy(stage_dn, dns.at[l, span(f, TILE), :], sem_out.at[2]))

    def late_copy(f, slot, act, back):
        ends = (late.at[f], dgu.at[slot]) if back else (dgu.at[slot], late.at[f])
        act(pltpu.make_async_copy(*ends, sem_late.at[slot]))

    def states_back(slot):
        half = TOKENS // 2

        @pl.loop(0, 2)
        def _(t):
            acc[span(t, half), :] += nt(dgu[slot, span(t, half), :], wgu_t[slot])

    def norm_back():
        @pl.loop(0, TOKENS // TILE)
        def _(t):
            rows = span(t, TILE)
            wide = hbuf[rows, :].astype(F32)
            s = scale_of(wide)
            n, by_a = wide * s, acc[rows, :]
            by_h = s * (by_a - n * jnp.mean(by_a * n, -1, keepdims=True))
            ct[rows, :] = (ct[rows, :].astype(F32) + by_h).astype(BF16)

    first = pltpu.make_async_copy(dy, ct, sem_h.at[0])
    first.start()
    pltpu.make_async_copy(h1, hbuf, sem_h.at[1]).start()
    inputs(0, 0, start)
    first.wait()

    def body(step):
        l, f, slot = 1 - step // TILES, lax.rem(step, TILES), lax.rem(step, 2)
        inputs(step, slot, wait)

        @pl.when(step + 1 < 2 * TILES)
        def _():
            inputs(step + 1, 1 - slot, start)

        @pl.when(f == 0)
        def _():
            pltpu.make_async_copy(h1, hbuf, sem_h.at[1]).wait()

            @pl.loop(0, TOKENS // TILE)
            def _(t):
                rows = span(t, TILE)
                wide = hbuf[rows, :].astype(F32)
                at[:, rows] = (wide * scale_of(wide)).T.astype(BF16)
                acc[rows, :] = jnp.zeros((TILE, D), F32)

        @pl.when(step > TILES + 1)
        def _():
            late_copy(f - 2, slot, wait, NO)

        @pl.loop(0, 2)
        def _(t):
            rows = span(t, TOKENS // 2)
            by_p = nt(ct[rows, :], wd_t[slot]).astype(BF16).astype(F32)
            dgu[slot, rows, pl.ds(0, TILE)] = (by_p * up[slot, rows, :]).astype(BF16)
            dgu[slot, rows, pl.ds(TILE, TILE)] = (by_p * gate[slot, rows, :]).astype(BF16)

        @pl.when(f > 0)
        def _():
            outputs(l, f - 1, wait)
        stage[ALL, ALL] = nn(at[ALL, ALL], dgu[slot]).astype(BF16)
        outputs(l, f, start)

        @pl.when(l == 0)
        def _():
            late_copy(f, slot, start, NO)

        @pl.when(l == 1)
        def _():
            @pl.when(f > 0)
            def _():
                down_output(l, f - 1, wait)
            stage_dn[ALL, ALL] = nn(p[slot], ct[ALL, ALL]).astype(BF16)
            down_output(l, f, start)
            states_back(slot)

        @pl.when(step == TILES - 1)
        def _():
            outputs(l, f, wait)
            launch(0)
            down_output(l, f, wait)
            launch(1)
            norm_back()
            pltpu.make_async_copy(h0, hbuf, sem_h.at[1]).start()
            ready(0)
            ready(1)

        for i in range(TILES):
            @pl.when(step == TILES + i)
            def _():
                clock.advance(GRADS_CLOCK[0] + (i + 1) * GRADS_CLOCK[1])

    repeat(2 * TILES, body)
    outputs(0, TILES - 1, wait)
    launch(2)
    for f in (TILES - 2, TILES - 1):
        late_copy(f, (f + TILES) % 2, wait, NO)

    def again(f, slot, act, which):
        if which:
            late_copy(f, slot, act, YES)
            for i in range(2):
                act(pltpu.make_async_copy(wgu.at[i, :, span(f, TILE)], wgu_t.at[slot, :, pl.ds(i * TILE, TILE)], sem_in.at[slot, i]))
        else:
            act(pltpu.make_async_copy(pt.at[0, span(f, TILE), :], p.at[slot], sem_in.at[slot, 2]))

    again(0, 0, start, NO)
    again(0, 0, start, YES)
    ready(2)

    def late_down(f):
        slot = lax.rem(f, 2)
        again(f, slot, wait, NO)

        @pl.when(f + 1 < TILES)
        def _():
            again(f + 1, 1 - slot, start, NO)

        @pl.when(f > 0)
        def _():
            down_output(0, f - 1, wait)
        stage_dn[ALL, ALL] = nn(p[slot], ct[ALL, ALL]).astype(BF16)
        down_output(0, f, start)
        for i in range(TILES):
            @pl.when(f == i)
            def _():
                clock.advance(LATE_DOWN_CLOCK[0] + (i + 1) * LATE_DOWN_CLOCK[1])
    repeat(TILES, late_down)
    down_output(0, TILES - 1, wait)
    launch(3)

    def late_states(f):
        slot = lax.rem(f, 2)
        again(f, slot, wait, YES)

        @pl.when(f + 1 < TILES)
        def _():
            again(f + 1, 1 - slot, start, YES)
        states_back(slot)

        @pl.when(f == 0)
        def _():
            ready(3)
        for i in range(TILES):
            @pl.when(f == i)
            def _():
                clock.advance(LATE_STATES_CLOCK[0] + (i + 1) * LATE_STATES_CLOCK[1])
    repeat(TILES, late_states)
    norm_back()
    last = pltpu.make_async_copy(ct, dx, sem_h.at[0])
    last.start()
    for i in range(len(collect)):
        clock.finish(i)
    for act in (start, wait):
        for one in collect:
            act(one[-1]())
    last.wait()


SCATTER_RECV = 43


def back(dy, h0, h1, wgu, wd, silu, slope, pt):
    hbm = pl.BlockSpec(memory_space=pl.ANY)
    vmem, dma = pltpu.VMEM, pltpu.SemaphoreType.DMA
    buffers = []
    for count, units, columns in ((2, GU_UNITS, FF), (1, DN_UNITS, D)):
        whole = vmem((count, NX, NY, NZ, units["all"], ROWS, columns), BF16)
        buffers += [whole, whole, *(vmem((count, ARRIVALS, units[colour][1], ROWS, columns), BF16) for colour in "ABC")]
    double, states = vmem((2, TOKENS, TILE), F32), vmem((TOKENS, D), BF16)
    return pl.pallas_call(
        back_kernel, name="back",
        out_shape=(jax.ShapeDtypeStruct((TOKENS, D), BF16), jax.ShapeDtypeStruct((2 * LAYERS, GU_UNITS["all"], ROWS, FF), BF16),
                   jax.ShapeDtypeStruct((LAYERS, DN_UNITS["all"], ROWS, D), BF16), jax.ShapeDtypeStruct((2 * LAYERS, D, FF), BF16),
                   jax.ShapeDtypeStruct((LAYERS, FF, D), BF16), jax.ShapeDtypeStruct((TILES, TOKENS, 2 * TILE), BF16)),
        in_specs=[hbm] * 8, out_specs=(hbm,) * 6,
        scratch_shapes=[states, states, vmem((D, TOKENS), BF16), vmem((TOKENS, D), F32), double, double, vmem((2, D, 2 * TILE), BF16), vmem((2, TILE, D), BF16),
                        vmem((2, TILE, TOKENS), BF16), vmem((2, TOKENS, 2 * TILE), BF16), vmem((D, 2 * TILE), BF16), vmem((TILE, D), BF16), *buffers, *buffers,
                        dma((4, 4)), dma((4, SCATTER_RECV)), dma((2, 6)), dma((2,)), dma((3,)), dma((2,)), dma((4,))],
        compiler_params=pltpu.CompilerParams(collective_id=1, has_side_effects=YES, vmem_limit_bytes=LIMIT),
    )(dy, h0, h1, wgu, wd, silu, slope, pt)[:3]


def solution(mesh):
    def step(x, dy, w_gate, w_up, w_down):
        gu_in = jnp.stack([w_gate, w_up], 1).reshape(2 * LAYERS, GU_UNITS["all"], ROWS, FF)
        x, dy = x[0], dy[0]
        gu, dn, h, silu, slope, pt = forward(x, gu_in, w_down.reshape(LAYERS, DN_UNITS["all"], ROWS, D))
        dx, by_gu, by_dn = back(dy, x, h, gu.reshape(2 * LAYERS, D, FF), dn.reshape(LAYERS, FF, D), silu, slope, pt)
        by_gu = by_gu.reshape(w_gate.shape[0], 2, *w_gate.shape[1:])
        return dx[None], by_gu[:, 0], by_gu[:, 1], by_dn.reshape(w_down.shape)

    rows = P(None, "dp", None)
    tokens, grads = P(("rep", "dp"), None, None), P("rep", "dp", None)
    return jax.shard_map(step, mesh=mesh, in_specs=(tokens, tokens, rows, rows, rows), out_specs=(tokens, grads, grads, grads), check_vma=NO)
```
